32 devices in a mesh: pipe: 1, seq: 32 (over z, y, x, core).
Axes of the slice: x: 2, y: 2, z: 4, core: 2. Of those that a mesh axis runs over, the one named last changes fastest.
Arguments:
- inputs: bfloat16 [2, 16384, 512], P(None, 'seq'), may hold values from -6 to 6
- w_in: bfloat16 [1, 512, 2048], P('pipe'), may hold values from -0.25 to 0.25
- w_out: bfloat16 [1, 512, 512], P('pipe'), may hold values from -0.25 to 0.25
- lengths: int32 [2, 8], replicated, may hold values from 1 to 4096, 16384 in all within a row
- valid: int32 [2, 32], replicated, may hold values from 128 to 512
Outputs:
- states: bfloat16 [1, 2, 16384, 512], P('pipe', None, 'seq')
The draws below stay inside these ranges and needn't reach their ends.
Inputs may be any that keep to these rules, and one draw needn't show every extreme that they name: Each row of stream lengths sums to 16384.
All inputs are finite; a program needn't handle non-finite values.
Results may differ from the reference program's by a relative error of at most 0.025.
Values may be sent and summed in bfloat16 or wider, within the bound.
A program may use at most 64 MiB of HBM per device.

```python
import math
import jax
import jax.numpy as jnp
import numpy as np
from jax import lax

D = 512
HEADS = 4
HEAD_DIM = 128
WINDOW = 512
MICRO = 2
TOK_DEV = 512
HD = 512
LAYERS = 1
ROWS = 16384
GROUPS = 32
STREAMS = 8


def place_ends(array, stream_key, low, top_value):
    longest = array.shape.index(max(array.shape))
    spots = []
    for shift in (0, 1):
        where = [jax.random.randint(jax.random.fold_in(stream_key, axis), (), 0, length) for axis, length in enumerate(array.shape)]
        where[longest] = (where[longest] + shift) % array.shape[longest]
        spots.append(tuple(where))
    return array.at[spots[0]].set(low).at[spots[1]].set(top_value)


def steps_of(own_key, shape, pieces, smallest, top_value):
    factor_of = 1.0
    for axis_at, shards_of in pieces:
        steps = jax.random.uniform(jax.random.fold_in(jax.random.fold_in(own_key, 6), axis_at), (shards_of,), jnp.float32, smallest / len(pieces), top_value / len(pieces))
        factor_of = factor_of * jnp.repeat(jnp.exp(steps), shape[axis_at] // shards_of).reshape((-1,) + (1,) * (len(shape) - 1 - axis_at))
    return factor_of


def profile(number_of, total, limit, slope):
    portions = [(1 << 20) // math.isqrt(grade ** slope) + 1 for grade in range(2, number_of + 1)]
    surplus, holding = total - limit - (number_of - 1), [1] * (number_of - 1)
    while surplus > 0:
        candidates = [i for i in range(number_of - 1) if holding[i] < limit]
        pool, left = sum([portions[i] for i in candidates]), surplus
        for i in candidates:
            extra = min(limit - holding[i], max(1, left * portions[i] // pool), surplus)
            holding[i] = holding[i] + extra
            surplus = surplus - extra
    return np.array([limit] + holding)


def uneven(key, count, total, reach, skew):
    if count == 2:
        one = jax.random.randint(key, (), max(1, total - reach), min(reach, total - 1) + 1)
        return jnp.stack([one, total - one])
    tallies = jnp.asarray(profile(count, total, reach, skew), jnp.int32)
    pairs = (count - 1) // 2
    donor, sink = tallies[1:1 + 2 * pairs:2], tallies[2:2 + 2 * pairs:2]
    slack = jnp.minimum(donor - 1, reach - sink)
    moved = jax.random.randint(jax.random.fold_in(key, 1), (pairs,), 0, 1 << 20) % (slack + 1)
    tallies = tallies.at[1:1 + 2 * pairs:2].set(donor - moved).at[2:2 + 2 * pairs:2].set(sink + moved)
    return tallies[jax.random.permutation(jax.random.fold_in(key, 2), count)]


def scatter_about(key, shape, scale, bound, cuts=(), held_as=jnp.bfloat16):
    entries = jax.random.normal(key, shape, jnp.float32) * scale
    if len(cuts) > 0:
        entries = steps_of(key, shape, cuts, -0.22, 0.18) * entries
    return jnp.clip(entries, min=-bound, max=bound).astype(held_as)


def setup_inputs(seed: int = 0) -> dict:
    splits = jax.random.split(jax.random.key(seed), 6)
    return {
        "inputs": scatter_about(splits[0], (MICRO, ROWS, D), 1.0, 6.0, ((1, 32),)),
        "w_in": scatter_about(splits[1], (LAYERS, D, 4 * HD), D ** -0.5, 0.25),
        "w_out": scatter_about(splits[2], (LAYERS, HD, D), HD ** -0.5, 0.25),
        "lengths": jax.vmap(lambda own: uneven(own, STREAMS, ROWS, ROWS // 4, 2))(jax.random.split(splits[3], MICRO)).reshape((MICRO, STREAMS)).astype(jnp.int32),
        "valid": place_ends(jax.random.randint(splits[4], (MICRO, GROUPS), TOK_DEV // 4, TOK_DEV + 1), jax.random.fold_in(splits[4], 1), TOK_DEV // 4, TOK_DEV).astype(jnp.int32),
    }


norm_eps = 1e-05
out_eps = 0.001

def layer_norm(values, epsilon):
    mean = lax.optimization_barrier(jnp.mean(values, axis=-1, keepdims=True))
    centred = values - mean
    spread = lax.optimization_barrier(jnp.mean(centred * centred, axis=-1, keepdims=True))
    return centred / jnp.sqrt(spread + epsilon)

def one_layer(hidden, weight_in, weight_out, bounds, valid_row):
    rows = hidden.shape[0]
    width = HEADS * HEAD_DIM
    normed = layer_norm(hidden.astype(jnp.float32), norm_eps).astype(jnp.bfloat16)
    proj = jax.nn.silu(jnp.dot(normed, weight_in, preferred_element_type=jnp.float32)).astype(jnp.bfloat16)
    gate_part = proj[:, :width]
    value_part = proj[:, width:2 * width]
    query_part = proj[:, 2 * width:3 * width]
    key_part = proj[:, 3 * width:]
    places = jnp.arange(rows, dtype=jnp.int32)
    stream = lax.optimization_barrier(jnp.sum((places[:, None] >= bounds[None, :]).astype(jnp.int32), axis=1))
    live = places % TOK_DEV < valid_row[places // TOK_DEV]
    key_pad = jnp.concatenate([jnp.zeros((WINDOW, width), key_part.dtype), key_part], 0)
    value_pad = jnp.concatenate([jnp.zeros((WINDOW, width), value_part.dtype), value_part], 0)
    stream_pad = jnp.concatenate([jnp.zeros((WINDOW,), jnp.int32) - 1, stream], 0)
    live_pad = jnp.concatenate([jnp.zeros((WINDOW,), bool), live], 0)
    span = TOK_DEV + WINDOW
    score_scale = 1.0 / math.sqrt(HEAD_DIM)
    mix_scale = 1.0 / math.sqrt(WINDOW)

    def block(index):
        start = (index * TOK_DEV).astype(jnp.int32)
        query = lax.dynamic_slice_in_dim(query_part, start, TOK_DEV, 0).astype(jnp.float32)
        keys = lax.dynamic_slice_in_dim(key_pad, start, span, 0).astype(jnp.float32)
        values = lax.dynamic_slice_in_dim(value_pad, start, span, 0).astype(jnp.float32)
        query_stream = lax.dynamic_slice_in_dim(stream, start, TOK_DEV, 0)
        key_stream = lax.dynamic_slice_in_dim(stream_pad, start, span, 0)
        query_live = lax.dynamic_slice_in_dim(live, start, TOK_DEV, 0)
        key_live = lax.dynamic_slice_in_dim(live_pad, start, span, 0)
        query_pos = start + jnp.arange(TOK_DEV, dtype=jnp.int32)
        key_pos = start - WINDOW + jnp.arange(span, dtype=jnp.int32)
        allowed = query_live[:, None] & key_live[None, :] & (query_stream[:, None] == key_stream[None, :]) & (key_pos[None, :] <= query_pos[:, None]) & (query_pos[:, None] - key_pos[None, :] < WINDOW) & (key_pos[None, :] >= 0)
        scores = jnp.einsum('qhd,khd->hqk', query.reshape(TOK_DEV, HEADS, HEAD_DIM), keys.reshape(span, HEADS, HEAD_DIM))
        weights = jnp.where(allowed[None], jax.nn.silu(scores * score_scale) * mix_scale, 0.0).astype(jnp.bfloat16)
        mixed = jnp.einsum('hqk,khd->qhd', weights.astype(jnp.float32), values.reshape(span, HEADS, HEAD_DIM))
        return mixed.reshape(TOK_DEV, width)
    attended = lax.map(block, jnp.arange(rows // TOK_DEV, dtype=jnp.int32)).reshape(rows, width)
    gated = (layer_norm(attended, out_eps) * gate_part.astype(jnp.float32)).astype(jnp.bfloat16)
    return (hidden.astype(jnp.float32) + jnp.dot(gated, weight_out, preferred_element_type=jnp.float32)).astype(jnp.bfloat16)

def reference(inputs, w_in, w_out, lengths, valid):
    results = []
    current = [inputs[m] for m in range(MICRO)]
    for layer in range(LAYERS):
        outputs = []
        for m in range(MICRO):
            bounds = jnp.cumsum(lengths[m]).astype(jnp.int32)
            outputs.append(one_layer(current[m], w_in[layer], w_out[layer], bounds, valid[m]))
        results.append(jnp.stack(outputs, 0))
        current = outputs
    return jnp.stack(results, 0)
```

```python
import functools
import math

import jax
import jax.numpy as jnp
from jax import lax
from jax.experimental import pallas as pl
from jax.experimental.pallas import tpu as pltpu
from jax.sharding import PartitionSpec as P

HEAD_DIM = 128
WINDOW = 512
TILE = 256
LANES = 128
PARTS = 3
HEADS_AT_ONCE = 4

norm_eps = 1e-05
out_eps = 0.001

score_scale = 1.0 / math.sqrt(HEAD_DIM)
mix_scale = 1.0 / math.sqrt(WINDOW)
fold = score_scale * mix_scale * 0.5
inner = 1.0 / mix_scale


def normalise(values, epsilon):
    mean = jnp.mean(values, axis=-1, keepdims=True)
    centred = values - mean
    spread = jnp.mean(centred * centred, axis=-1, keepdims=True)
    return centred * lax.rsqrt(spread + epsilon)


def silu(v):
    half = v * 0.5
    return half + half * jnp.tanh(half)


def layer_kernel(
    micro, size,
    x_hbm, win_hbm, wout_hbm, len_hbm, val_hbm, out_v,
    x_v, xr_v, win_v, wout_v, norm_v, u_v, v_v, q_v, k_v, kp_v, vp_v, acc_v, lo_v, len_ref, val_ref,
    load_sem, weight_sem, scalar_sem, send_sem, recv_sem,
):
    block = lax.axis_index("seq")
    barrier = pltpu.get_barrier_semaphore()

    @pl.when(block > 0)
    def _():
        pl.semaphore_signal(
            barrier, inc=1, device_id={"seq": block - 1}, device_id_type=pl.DeviceIdType.MESH
        )

    tok, width = x_v.shape[1], x_v.shape[2]
    branch = wout_v.shape[0]
    heads = branch // HEAD_DIM
    streams = len_ref.shape[1]
    f32 = jnp.float32
    bf16 = jnp.bfloat16

    loads = [
        pltpu.make_async_copy(x_hbm.at[m], x_v.at[m], load_sem.at[m]) for m in range(micro)
    ]
    weights = [
        pltpu.make_async_copy(
            win_hbm.at[0, :, pl.ds(c * branch, branch)], win_v.at[c], weight_sem.at[c]
        )
        for c in range(4)
    ]
    weights.append(pltpu.make_async_copy(wout_hbm.at[0], wout_v, weight_sem.at[4]))
    scalars = [
        pltpu.make_async_copy(len_hbm, len_ref, scalar_sem.at[0]),
        pltpu.make_async_copy(val_hbm, val_ref, scalar_sem.at[1]),
    ]
    for copy in loads + scalars + weights:
        copy.start()

    def parts(m):
        half, quarter = tok // 2, tok // 4
        if m < micro - 1:
            return [(0, tok)]
        return [(half, tok), (quarter, half), (0, quarter)]

    def sends(m, p):
        first, last = parts(m)[p]
        rows = pl.ds(first, last - first)
        return pltpu.make_async_remote_copy(
            src_ref=x_v.at[m, rows, :],
            dst_ref=xr_v.at[m, rows, :],
            send_sem=send_sem.at[m, p],
            recv_sem=recv_sem.at[m, p],
            device_id={"seq": block + 1},
            device_id_type=pl.DeviceIdType.MESH,
        )

    for m in range(micro):
        loads[m].wait()

        @pl.when(block < size - 1)
        def _():
            if m == 0:
                pl.semaphore_wait(barrier, 1)
            for p in range(len(parts(m))):
                sends(m, p).start()

    @pl.when(block == 0)
    def _():
        xr_v[...] = jnp.zeros_like(xr_v)

    for copy in scalars:
        copy.wait()
    row = lax.broadcasted_iota(jnp.int32, (tok, LANES), 0)
    for m in range(micro):
        place = row + block * tok
        start = jnp.zeros((tok, LANES), jnp.int32)
        bound = jnp.int32(0)
        for k in range(streams):
            bound = bound + len_ref[m, k]
            start = jnp.where(place >= bound, bound, start)
        lo_v[m] = start - block * tok

    def norm_rows(source, m, first=0, last=None):
        for at in range(first, tok if last is None else last, 128):
            rows = slice(at, at + 128)
            norm_v[rows, :] = normalise(source[m, rows, :].astype(f32), norm_eps).astype(bf16)

    live_row = lax.broadcasted_iota(jnp.int32, (tok, branch), 0)

    def project(c):
        return jnp.dot(norm_v[...], win_v[c], preferred_element_type=f32)

    def weigh(query, keys, keep):
        s = lax.dot_general(query, keys, (((1,), (1,)), ((), ())), preferred_element_type=f32)
        a = s + s * jnp.tanh(s * inner)
        return jnp.where(keep, a, 0.0).astype(bf16)

    def attend(m, previous, top=0, end=None):
        end = tok if end is None else end
        tile = min(TILE, end - top)
        key_ref, value_ref = (kp_v, vp_v) if previous else (k_v, v_v)

        def group(g, carry):
            plans = []
            for i in range(HEADS_AT_ONCE):
                cols = pl.ds(
                    pl.multiple_of((g * HEADS_AT_ONCE + i) * HEAD_DIM, HEAD_DIM), HEAD_DIM
                )
                for at in range(top, end, tile):
                    rows = slice(at, at + tile)
                    first, last = (at, tok) if previous else (0, at + tile)
                    span = slice(first, last)
                    shape = (tile, last - first)
                    low = jnp.concatenate([lo_v[m, rows, :]] * (shape[1] // LANES), 1)
                    place = lax.broadcasted_iota(jnp.int32, shape, 1) + first
                    line = lax.broadcasted_iota(jnp.int32, shape, 0) + at
                    if previous:
                        keep = (place - tok >= low) & (place > line)
                    else:
                        keep = (place >= low) & (place <= line)
                    plans.append((rows, cols, span, keep))
            parts = [weigh(q_v[m, r, c], key_ref[k, c], keep) for r, c, k, keep in plans]
            for (r, c, k, _), a in zip(plans, parts):
                part = jnp.dot(a, value_ref[k, c], preferred_element_type=f32)
                acc_v[m, r, c] = acc_v[m, r, c] + part if previous else part
            return carry

        lax.fori_loop(0, heads // HEADS_AT_ONCE, group, 0)

    for m in range(micro):
        norm_rows(x_v, m)
        count = val_ref[m, block]
        for c in range(4):
            if m == 0:
                weights[c].wait()
            part = silu(project(c))
            if c == 0:
                u_v[m] = part.astype(bf16)
            elif c == 1:
                v_v[...] = jnp.where(live_row < count, part, 0.0).astype(bf16)
            elif c == 2:
                q_v[m] = (part.astype(bf16).astype(f32) * fold).astype(bf16)
            else:
                k_v[...] = part.astype(bf16)
        attend(m, False)

    weights[4].wait()
    for m in range(micro):
        before = jnp.where(block > 0, val_ref[m, jnp.maximum(block - 1, 0)], 0)
        count = val_ref[m, block]
        for p in range(len(parts(m))):
            first, last = parts(m)[p]
            rows = slice(first, last)

            @pl.when(block > 0)
            def _():
                sends(m, p).wait_recv()

            norm_rows(xr_v, m, first, last)
            normed = norm_v[rows, :]
            value = silu(jnp.dot(normed, win_v[1], preferred_element_type=f32))
            vp_v[rows, :] = jnp.where(live_row[: last - first] + first < before, value, 0.0).astype(bf16)
            kp_v[rows, :] = silu(jnp.dot(normed, win_v[3], preferred_element_type=f32)).astype(bf16)
            attend(m, True, first, last)
            for at in range(first, last, 128):
                rows = slice(at, at + 128)
                gated = normalise(acc_v[m, rows, :], out_eps) * u_v[m, rows, :].astype(f32)
                gated = jnp.where(live_row[:128] + at < count, gated, 0.0).astype(bf16)
                out_v[m, rows, :] = (
                    x_v[m, rows, :].astype(f32)
                    + jnp.dot(gated, wout_v[...], preferred_element_type=f32)
                ).astype(bf16)
    for m in range(micro):
        @pl.when(block < size - 1)
        def _():
            for p in range(len(parts(m))):
                sends(m, p).wait_send()


def layer(x, w_in, w_out, lengths, valid):
    micro, tok, width = x.shape
    branch = w_out.shape[1]
    size = lax.axis_size("seq")
    assert tok == WINDOW
    bf16 = jnp.bfloat16
    anywhere = pl.BlockSpec(memory_space=pl.ANY)
    return pl.pallas_call(
        functools.partial(layer_kernel, micro, size),
        out_shape=pltpu.VMEM((micro, tok, width), bf16),
        in_specs=[anywhere] * 5,
        out_specs=pl.BlockSpec(memory_space=pltpu.VMEM),
        scratch_shapes=[
            pltpu.VMEM((micro, tok, width), bf16),
            pltpu.VMEM((micro, tok, width), bf16),
            pltpu.VMEM((4, width, branch), bf16),
            pltpu.VMEM((branch, width), bf16),
            pltpu.VMEM((tok, width), bf16),
            pltpu.VMEM((micro, tok, branch), bf16),
            pltpu.VMEM((tok, branch), bf16),
            pltpu.VMEM((micro, tok, branch), bf16),
            pltpu.VMEM((tok, branch), bf16),
            pltpu.VMEM((tok, branch), bf16),
            pltpu.VMEM((tok, branch), bf16),
            pltpu.VMEM((micro, tok, branch), jnp.float32),
            pltpu.VMEM((micro, tok, LANES), jnp.int32),
            pltpu.SMEM(lengths.shape, jnp.int32),
            pltpu.SMEM(valid.shape, jnp.int32),
            pltpu.SemaphoreType.DMA((micro,)),
            pltpu.SemaphoreType.DMA((5,)),
            pltpu.SemaphoreType.DMA((2,)),
            pltpu.SemaphoreType.DMA((micro, PARTS)),
            pltpu.SemaphoreType.DMA((micro, PARTS)),
        ],
        compiler_params=pltpu.CompilerParams(
            collective_id=0, has_side_effects=True, vmem_limit_bytes=56 * 1024 * 1024
        ),
    )(x, w_in, w_out, lengths, valid)


def shards(inputs, w_in, w_out, lengths, valid):
    micro, tok, width = inputs.shape
    sections = lax.axis_size("pipe")
    if sections == 1:
        return layer(inputs, w_in, w_out, lengths, valid)[None]

    section = lax.axis_index("pipe")
    pairs = [(i, i + 1) for i in range(sections - 1)]

    def tick(step, carry):
        incoming, states = carry
        slot = step - section
        active = (slot >= 0) & (slot < micro)
        index = jnp.clip(slot, 0, micro - 1)
        fresh = lax.dynamic_index_in_dim(inputs, index, 0, keepdims=True)
        x_rows = jnp.where(section == 0, fresh, incoming)
        result = layer(
            x_rows,
            w_in,
            w_out,
            lax.dynamic_index_in_dim(lengths, index, 0, keepdims=True),
            lax.dynamic_index_in_dim(valid, index, 0, keepdims=True),
        )
        zero = jnp.zeros((), jnp.int32)
        updated = lax.dynamic_update_slice(states, result[None], (zero, index, zero, zero))
        states = jnp.where(active, updated, states)
        return (lax.ppermute(result, "pipe", pairs), states)

    start = (
        jnp.zeros((1, tok, width), jnp.bfloat16),
        jnp.zeros((1, micro, tok, width), jnp.bfloat16),
    )
    return lax.fori_loop(0, sections + micro - 1, tick, start)[1]


def solution(mesh):
    in_specs = (P(None, "seq", None), P("pipe", None, None), P("pipe", None, None), P(), P())
    out_specs = P("pipe", None, "seq", None)
    return jax.shard_map(shards, mesh=mesh, in_specs=in_specs, out_specs=out_specs, check_vma=False)
```

```python
import functools
import math

import jax
import jax.numpy as jnp
from jax import lax
from jax.experimental import pallas as pl
from jax.experimental.pallas import tpu as pltpu
from jax.sharding import PartitionSpec as P

HEAD_DIM = 128
WINDOW = 512
TILE = 256
LANES = 128
PARTS = 3
PLANE = 8
DETOUR = 80

norm_eps = 1e-05
out_eps = 0.001

score_scale = 1.0 / math.sqrt(HEAD_DIM)
fold = score_scale * 0.5
mixed_eps = out_eps * WINDOW


def normalise(values, epsilon):
    mean = jnp.mean(values, axis=-1, keepdims=True)
    centred = values - mean
    spread = jnp.mean(centred * centred, axis=-1, keepdims=True)
    return centred * lax.rsqrt(spread + epsilon)


def silu(v):
    half = v * 0.5
    return half + half * jnp.tanh(half)


def layer_kernel(
    micro, size, detours,
    x_hbm, win_hbm, wout_hbm, len_hbm, val_hbm, out_v,
    x_v, xr_v, win_v, wout_v, norm_v, u_v, v_v, q_v, k_v, kp_v, vp_v, acc_v, lo_v, len_ref, val_ref, detour_v,
    load_sem, weight_sem, scalar_sem, send_sem, recv_sem, detour_sem,
):
    block = lax.axis_index("seq")
    barrier = pltpu.get_barrier_semaphore()

    def greet(when, device):
        @pl.when(when)
        def _():
            pl.semaphore_signal(
                barrier, inc=1, device_id={"seq": device}, device_id_type=pl.DeviceIdType.MESH
            )

    greet(block > 0, block - 1)
    detour_of = [
        (z * PLANE + PLANE - 1, 0, z * PLANE + PLANE, z * DETOUR)
        for z in range(detours)
    ]
    for source, via, target, _ in detour_of:
        greet(block == target, via)
        greet(block == via, source)

    tok, width = x_v.shape[1], x_v.shape[2]
    branch = wout_v.shape[0]
    heads = branch // HEAD_DIM
    streams = len_ref.shape[1]
    f32 = jnp.float32
    bf16 = jnp.bfloat16

    loads = [
        pltpu.make_async_copy(x_hbm.at[m], x_v.at[m], load_sem.at[m]) for m in range(micro)
    ]
    weights = [
        pltpu.make_async_copy(
            win_hbm.at[0, :, pl.ds(c * branch, branch)], win_v.at[c], weight_sem.at[c]
        )
        for c in range(4)
    ]
    weights.append(pltpu.make_async_copy(wout_hbm.at[0], wout_v, weight_sem.at[4]))
    scalars = [
        pltpu.make_async_copy(len_hbm, len_ref, scalar_sem.at[0]),
        pltpu.make_async_copy(val_hbm, val_ref, scalar_sem.at[1]),
    ]
    for copy in loads + scalars + weights:
        copy.start()

    def parts(m):
        half, quarter = tok // 2, tok // 4
        if m < micro - 1:
            return [(half, tok), (0, half)]
        return [(half, tok), (quarter, half), (0, quarter)]

    def remote(src, dst, send, recv, device):
        return pltpu.make_async_remote_copy(
            src_ref=src,
            dst_ref=dst,
            send_sem=send,
            recv_sem=recv,
            device_id={"seq": device},
            device_id_type=pl.DeviceIdType.MESH,
        )

    def sends(m, p, cut=0):
        first, last = parts(m)[p]
        rows = pl.ds(first, last - cut - first)
        return remote(
            x_v.at[m, rows, :], xr_v.at[m, rows, :], send_sem.at[m, p], recv_sem.at[m, p], block + 1
        )

    final = micro - 1

    def leave(via, slot):
        rows = pl.ds(tok - DETOUR, DETOUR)
        return remote(
            x_v.at[final, rows, :], detour_v.at[pl.ds(slot, DETOUR), :],
            detour_sem.at[0], detour_sem.at[1 + slot // DETOUR], via,
        )

    def forward(target, slot):
        rows = pl.ds(tok - DETOUR, DETOUR)
        return remote(
            detour_v.at[pl.ds(slot, DETOUR), :], xr_v.at[final, rows, :],
            detour_sem.at[1 + detours + slot // DETOUR], detour_sem.at[1 + 2 * detours], target,
        )

    def route(when, m, p, act, end):
        plain = when
        if (m, p) == (final, 0):
            for source, via, target, slot in detour_of:
                here = block == (source if end == 0 else target)
                plain = plain & jnp.logical_not(here)

                @pl.when(here)
                def _():
                    act(sends(m, p, DETOUR))
                    if end:
                        act(forward(target, slot))

        @pl.when(plain)
        def _():
            act(sends(m, p))

    early = block < size - 1
    if detours:
        early = early & (block > 0)

    for m in range(micro):
        if m == 0:
            for copy in loads:
                copy.wait()
            one = early
            for source, _, _, _ in detour_of:
                one = one & (block != source)

                @pl.when(block == source)
                def _():
                    pl.semaphore_wait(barrier, 2)

            @pl.when(one)
            def _():
                pl.semaphore_wait(barrier, 1)

            for source, via, _, slot in detour_of:
                @pl.when(block == source)
                def _():
                    leave(via, slot).start()

        if m == final:
            pass
        for p in range(len(parts(m))):
            route(early, m, p, lambda copy: copy.start(), 0)

    @pl.when(block == 0)
    def _():
        xr_v[...] = jnp.zeros_like(xr_v)

    for copy in scalars + weights:
        copy.wait()
    row = lax.broadcasted_iota(jnp.int32, (tok, LANES), 0)
    for m in range(micro):
        place = row + block * tok
        start = jnp.zeros((tok, LANES), jnp.int32)
        bound = jnp.int32(0)
        for k in range(streams):
            bound = bound + len_ref[m, k]
            start = jnp.where(place >= bound, bound, start)
        lo_v[m] = start - block * tok

    def norm_rows(source, m, first=0, last=None):
        for at in range(first, tok if last is None else last, 128):
            rows = slice(at, at + 128)
            norm_v[rows, :] = normalise(source[m, rows, :].astype(f32), norm_eps).astype(bf16)

    live_row = lax.broadcasted_iota(jnp.int32, (tok, branch), 0)

    def project(c):
        return jnp.dot(norm_v[...], win_v[c], preferred_element_type=f32)

    def mask(m, previous, at, end, first, last):
        shape = (end - at, last - first)
        low = jnp.concatenate([lo_v[m, at:end, :]] * (shape[1] // LANES), 1)
        place = lax.broadcasted_iota(jnp.int32, shape, 1) + (first - tok if previous else first)
        keep = place >= low
        line = lax.broadcasted_iota(jnp.int32, shape, 0) + at
        if previous:
            return keep & (place > line - tok) if first < end else keep
        return keep & (place <= line) if last > at else keep

    def weigh(query, keys, keep):
        s = lax.dot_general(query, keys, (((1,), (1,)), ((), ())), preferred_element_type=f32)
        return jnp.where(keep, s + s * jnp.tanh(s), 0.0).astype(bf16)

    def attend(m, previous, blocks):
        key_ref, value_ref = (kp_v, vp_v) if previous else (k_v, v_v)
        plans = []
        for h in range(heads):
            cols = slice(h * HEAD_DIM, (h + 1) * HEAD_DIM)
            for at, end, first, last in blocks:
                keep = mask(m, previous, at, end, first, last)
                plans.append((slice(at, end), cols, slice(first, last), keep))
        weights = [weigh(q_v[m, r, c], key_ref[k, c], keep) for r, c, k, keep in plans]
        for (r, c, k, _), a in zip(plans, weights):
            part = jnp.dot(a, value_ref[k, c], preferred_element_type=f32)
            acc_v[m, r, c] = acc_v[m, r, c] + part if previous else part

    for m in range(micro):
        norm_rows(x_v, m)
        count = val_ref[m, block]
        for c in range(4):
            part = silu(project(c))
            if c == 0:
                u_v[m] = part.astype(bf16)
            elif c == 1:
                v_v[...] = jnp.where(live_row < count, part, 0.0).astype(bf16)
            elif c == 2:
                q_v[m] = (part.astype(bf16).astype(f32) * fold).astype(bf16)
            else:
                k_v[...] = part.astype(bf16)
        attend(m, False, [(at, at + TILE, 0, at + TILE) for at in range(0, tok, TILE)])

    if detours:
        @pl.when(block == 0)
        def _():
            pl.semaphore_wait(barrier, 1 + detours)
            for m in range(micro):
                for p in range(len(parts(m))):
                    sends(m, p).start()
            for _, _, target, slot in detour_of:
                leave(0, slot).wait_recv()
                forward(target, slot).start()

    def finish(m, first, last):
        count = val_ref[m, block]
        for at in range(first, last, 128):
            rows = slice(at, at + 128)
            gated = normalise(acc_v[m, rows, :], mixed_eps) * u_v[m, rows, :].astype(f32)
            gated = jnp.where(live_row[:128] + at < count, gated, 0.0).astype(bf16)
            out_v[m, rows, :] = (
                x_v[m, rows, :].astype(f32)
                + jnp.dot(gated, wout_v[...], preferred_element_type=f32)
            ).astype(bf16)

    ready = []
    for m in range(micro):
        before = jnp.where(block > 0, val_ref[m, jnp.maximum(block - 1, 0)], 0)
        for p in range(len(parts(m))):
            first, last = parts(m)[p]
            rows = slice(first, last)

            route(block > 0, m, p, lambda copy: copy.wait_recv(), 1)

            norm_rows(xr_v, m, first, last)
            normed = norm_v[rows, :]
            value = silu(jnp.dot(normed, win_v[1], preferred_element_type=f32))
            vp_v[rows, :] = jnp.where(live_row[: last - first] + first < before, value, 0.0).astype(bf16)
            kp_v[rows, :] = silu(jnp.dot(normed, win_v[3], preferred_element_type=f32)).astype(bf16)
            ahead = [(at, min(at + TILE, first), first, last) for at in range(0, first, TILE)]
            own = [(at, min(at + TILE, last), at, last) for at in range(first, last, TILE)]
            attend(m, True, own + ahead)
            for done in ready:
                finish(*done)
            ready = [(m, first, last)]
    for done in ready:
        finish(*done)
    for m in range(micro):
        for p in range(len(parts(m))):
            route(block < size - 1, m, p, lambda copy: copy.wait_send(), 0)
    for source, via, target, slot in detour_of:
        @pl.when(block == source)
        def _():
            leave(via, slot).wait_send()

        @pl.when(block == via)
        def _():
            forward(target, slot).wait_send()


def layer(x, w_in, w_out, lengths, valid):
    micro, tok, width = x.shape
    branch = w_out.shape[1]
    size = lax.axis_size("seq")
    assert tok == WINDOW
    planes = size // PLANE if lax.axis_size("pipe") == 1 else 0
    detours = max(planes - 1, 0)
    bf16 = jnp.bfloat16
    anywhere = pl.BlockSpec(memory_space=pl.ANY)
    return pl.pallas_call(
        functools.partial(layer_kernel, micro, size, detours),
        out_shape=pltpu.VMEM((micro, tok, width), bf16),
        in_specs=[anywhere] * 5,
        out_specs=pl.BlockSpec(memory_space=pltpu.VMEM),
        scratch_shapes=[
            pltpu.VMEM((micro, tok, width), bf16),
            pltpu.VMEM((micro, tok, width), bf16),
            pltpu.VMEM((4, width, branch), bf16),
            pltpu.VMEM((branch, width), bf16),
            pltpu.VMEM((tok, width), bf16),
            pltpu.VMEM((micro, tok, branch), bf16),
            pltpu.VMEM((tok, branch), bf16),
            pltpu.VMEM((micro, tok, branch), bf16),
            pltpu.VMEM((tok, branch), bf16),
            pltpu.VMEM((tok, branch), bf16),
            pltpu.VMEM((tok, branch), bf16),
            pltpu.VMEM((micro, tok, branch), jnp.float32),
            pltpu.VMEM((micro, tok, LANES), jnp.int32),
            pltpu.SMEM(lengths.shape, jnp.int32),
            pltpu.SMEM(valid.shape, jnp.int32),
            pltpu.VMEM((DETOUR * max(detours, 1), width), bf16),
            pltpu.SemaphoreType.DMA((micro,)),
            pltpu.SemaphoreType.DMA((5,)),
            pltpu.SemaphoreType.DMA((2,)),
            pltpu.SemaphoreType.DMA((micro, PARTS)),
            pltpu.SemaphoreType.DMA((micro, PARTS)),
            pltpu.SemaphoreType.DMA((2 + 2 * detours,)),
        ],
        compiler_params=pltpu.CompilerParams(
            collective_id=0, has_side_effects=True, vmem_limit_bytes=56 * 1024 * 1024
        ),
    )(x, w_in, w_out, lengths, valid)


def shards(inputs, w_in, w_out, lengths, valid):
    micro, tok, width = inputs.shape
    sections = lax.axis_size("pipe")
    if sections == 1:
        return layer(inputs, w_in, w_out, lengths, valid)[None]

    section = lax.axis_index("pipe")
    pairs = [(i, i + 1) for i in range(sections - 1)]

    def tick(step, carry):
        incoming, states = carry
        slot = step - section
        active = (slot >= 0) & (slot < micro)
        index = jnp.clip(slot, 0, micro - 1)
        fresh = lax.dynamic_index_in_dim(inputs, index, 0, keepdims=True)
        x_rows = jnp.where(section == 0, fresh, incoming)
        result = layer(
            x_rows,
            w_in,
            w_out,
            lax.dynamic_index_in_dim(lengths, index, 0, keepdims=True),
            lax.dynamic_index_in_dim(valid, index, 0, keepdims=True),
        )
        zero = jnp.zeros((), jnp.int32)
        updated = lax.dynamic_update_slice(states, result[None], (zero, index, zero, zero))
        states = jnp.where(active, updated, states)
        return (lax.ppermute(result, "pipe", pairs), states)

    start = (
        jnp.zeros((1, tok, width), jnp.bfloat16),
        jnp.zeros((1, micro, tok, width), jnp.bfloat16),
    )
    return lax.fori_loop(0, sections + micro - 1, tick, start)[1]


def solution(mesh):
    in_specs = (P(None, "seq", None), P("pipe", None, None), P("pipe", None, None), P(), P())
    out_specs = P("pipe", None, "seq", None)
    return jax.shard_map(shards, mesh=mesh, in_specs=in_specs, out_specs=out_specs, check_vma=False)
```

```python
import functools
import math

import jax
import jax.numpy as jnp
from jax import lax
from jax.experimental import pallas as pl
from jax.experimental.pallas import tpu as pltpu
from jax.sharding import PartitionSpec as P

HEAD_DIM = 128
WINDOW = 512
TILE = 256
LANES = 128
PARTS = 3
PLANE = 8
DETOUR = 80

norm_eps = 1e-05
out_eps = 0.001

score_scale = 1.0 / math.sqrt(HEAD_DIM)
fold = score_scale * 0.5
mixed_eps = out_eps * WINDOW


def normalise(values, epsilon):
    mean = jnp.mean(values, axis=-1, keepdims=True)
    centred = values - mean
    spread = jnp.mean(centred * centred, axis=-1, keepdims=True)
    return centred * lax.rsqrt(spread + epsilon)


def silu(v):
    half = v * 0.5
    return half + half * jnp.tanh(half)


def layer_kernel(
    micro, size, detours,
    x_hbm, win_hbm, wout_hbm, len_hbm, val_hbm, out_v,
    x_v, xr_v, win_v, wout_v, norm_v, u_v, v_v, q_v, k_v, kp_v, vp_v, acc_v, lo_v, len_ref, val_ref, detour_v, sum_v, gain_v,
    load_sem, weight_sem, scalar_sem, send_sem, recv_sem, detour_sem,
):
    block = lax.axis_index("seq")
    barrier = pltpu.get_barrier_semaphore()

    def greet(when, device):
        @pl.when(when)
        def _():
            pl.semaphore_signal(
                barrier, inc=1, device_id={"seq": device}, device_id_type=pl.DeviceIdType.MESH
            )

    greet(block > 0, block - 1)
    detour_of = [
        (z * PLANE + PLANE - 1, 0, z * PLANE + PLANE, z * DETOUR)
        for z in range(detours)
    ]
    for source, via, target, _ in detour_of:
        greet(block == target, via)
        greet(block == via, source)

    tok, width = x_v.shape[1], x_v.shape[2]
    branch = wout_v.shape[0]
    heads = branch // HEAD_DIM
    streams = len_ref.shape[1]
    f32 = jnp.float32
    bf16 = jnp.bfloat16

    loads = [
        pltpu.make_async_copy(x_hbm.at[m], x_v.at[m], load_sem.at[m]) for m in range(micro)
    ]
    weights = [
        pltpu.make_async_copy(
            win_hbm.at[0, :, pl.ds(c * branch, branch)], win_v.at[c], weight_sem.at[c]
        )
        for c in range(4)
    ]
    weights.append(pltpu.make_async_copy(wout_hbm.at[0], wout_v, weight_sem.at[4]))
    scalars = [
        pltpu.make_async_copy(len_hbm, len_ref, scalar_sem.at[0]),
        pltpu.make_async_copy(val_hbm, val_ref, scalar_sem.at[1]),
    ]
    for copy in loads + scalars + weights:
        copy.start()

    def parts(m):
        half, quarter = tok // 2, tok // 4
        if m < micro - 1:
            return [(half, tok), (0, half)]
        return [(half, tok), (quarter, half), (0, quarter)]

    def remote(src, dst, send, recv, device):
        return pltpu.make_async_remote_copy(
            src_ref=src,
            dst_ref=dst,
            send_sem=send,
            recv_sem=recv,
            device_id={"seq": device},
            device_id_type=pl.DeviceIdType.MESH,
        )

    def sends(m, p, cut=0):
        first, last = parts(m)[p]
        rows = pl.ds(first, last - cut - first)
        return remote(
            x_v.at[m, rows, :], xr_v.at[m, rows, :], send_sem.at[m, p], recv_sem.at[m, p], block + 1
        )

    final = micro - 1

    def leave(via, slot):
        rows = pl.ds(tok - DETOUR, DETOUR)
        return remote(
            x_v.at[final, rows, :], detour_v.at[pl.ds(slot, DETOUR), :],
            detour_sem.at[0], detour_sem.at[1 + slot // DETOUR], via,
        )

    def forward(target, slot):
        rows = pl.ds(tok - DETOUR, DETOUR)
        return remote(
            detour_v.at[pl.ds(slot, DETOUR), :], xr_v.at[final, rows, :],
            detour_sem.at[1 + detours + slot // DETOUR], detour_sem.at[1 + 2 * detours], target,
        )

    def route(when, m, p, act, end):
        plain = when
        if (m, p) == (final, 0):
            for source, via, target, slot in detour_of:
                here = block == (source if end == 0 else target)
                plain = plain & jnp.logical_not(here)

                @pl.when(here)
                def _():
                    act(sends(m, p, DETOUR))
                    if end:
                        act(forward(target, slot))

        @pl.when(plain)
        def _():
            act(sends(m, p))

    early = block < size - 1
    if detours:
        early = early & (block > 0)

    for m in range(micro):
        if m == 0:
            loads[0].wait()
            one = early
            for source, _, _, _ in detour_of:
                one = one & (block != source)

                @pl.when(block == source)
                def _():
                    pl.semaphore_wait(barrier, 2)

            @pl.when(one)
            def _():
                pl.semaphore_wait(barrier, 1)


        if m == final:
            pass
        if m > 0:
            loads[m].wait()
        if m == final:
            for source, via, _, slot in detour_of:
                @pl.when(block == source)
                def _():
                    leave(via, slot).start()

        for p in range(len(parts(m))):
            route(early, m, p, lambda copy: copy.start(), 0)

    @pl.when(block == 0)
    def _():
        xr_v[...] = jnp.zeros_like(xr_v)

    for copy in scalars + weights:
        copy.wait()
    row = lax.broadcasted_iota(jnp.int32, (tok, LANES), 0)
    for m in range(micro):
        place = row + block * tok
        start = jnp.zeros((tok, LANES), jnp.int32)
        bound = jnp.int32(0)
        for k in range(streams):
            bound = bound + len_ref[m, k]
            start = jnp.where(place >= bound, bound, start)
        lo_v[m] = start - block * tok

    def norm_rows(source, m, first=0, last=None):
        for at in range(first, tok if last is None else last, 128):
            rows = slice(at, at + 128)
            norm_v[rows, :] = normalise(source[m, rows, :].astype(f32), norm_eps).astype(bf16)

    live_row = lax.broadcasted_iota(jnp.int32, (tok, branch), 0)

    for c in (1, 3):
        ones = jnp.ones((8, width), bf16)
        sum_v[c] = jnp.dot(ones, win_v[c], preferred_element_type=f32)

    def project(c):
        return jnp.dot(norm_v[...], win_v[c], preferred_element_type=f32)

    def mask(m, previous, at, end, first, last):
        shape = (end - at, last - first)
        low = jnp.concatenate([lo_v[m, at:end, :]] * (shape[1] // LANES), 1)
        place = lax.broadcasted_iota(jnp.int32, shape, 1) + (first - tok if previous else first)
        keep = place >= low
        line = lax.broadcasted_iota(jnp.int32, shape, 0) + at
        if previous:
            return keep & (place > line - tok) if first < end else keep
        return keep & (place <= line) if last > at else keep

    def weigh(query, keys, keep):
        s = lax.dot_general(query, keys, (((1,), (1,)), ((), ())), preferred_element_type=f32)
        return jnp.where(keep, s + s * jnp.tanh(s), 0.0).astype(bf16)

    def attend(m, previous, blocks):
        key_ref, value_ref = (kp_v, vp_v) if previous else (k_v, v_v)
        plans = []
        for h in range(heads):
            cols = slice(h * HEAD_DIM, (h + 1) * HEAD_DIM)
            for at, end, first, last in blocks:
                keep = mask(m, previous, at, end, first, last)
                plans.append((slice(at, end), cols, slice(first, last), keep))
        weights = [weigh(q_v[m, r, c], key_ref[k, c], keep) for r, c, k, keep in plans]
        for (r, c, k, _), a in zip(plans, weights):
            part = jnp.dot(a, value_ref[k, c], preferred_element_type=f32)
            acc_v[m, r, c] = acc_v[m, r, c] + part if previous else part

    for m in range(micro):
        norm_rows(x_v, m)
        count = val_ref[m, block]
        for c in (2, 3, 1, 0):
            part = silu(project(c))
            if c == 0:
                u_v[m] = part.astype(bf16)
            elif c == 1:
                v_v[...] = jnp.where(live_row < count, part, 0.0).astype(bf16)
            elif c == 2:
                q_v[m] = (part.astype(bf16).astype(f32) * fold).astype(bf16)
            else:
                k_v[...] = part.astype(bf16)
        attend(m, False, [(at, at + TILE, 0, at + TILE) for at in range(0, tok, TILE)])

    if detours:
        @pl.when(block == 0)
        def _():
            pl.semaphore_wait(barrier, 1 + detours)
            for m in range(micro):
                for p in range(len(parts(m))):
                    sends(m, p).start()
            for _, _, target, slot in detour_of:
                leave(0, slot).wait_recv()
                forward(target, slot).start()

    def raw_projection(rows):
        raw = rows.astype(f32)
        mean = jnp.mean(raw, axis=-1, keepdims=True)
        centred = raw - mean
        scale = lax.rsqrt(jnp.mean(centred * centred, axis=-1, keepdims=True) + norm_eps)

        def part(c):
            product = jnp.dot(rows, win_v[c], preferred_element_type=f32)
            return scale * (product - mean * sum_v[c, 0:1, :])

        return part

    def prepare(m, last):
        rows = slice(0, last)
        acc = acc_v[m, rows, :]
        acc_v[m, rows, :] = acc - jnp.mean(acc, axis=-1, keepdims=True)
        gain_v[...] = jnp.dot(u_v[m, rows, :], wout_v[...], preferred_element_type=f32)

    def finish_last(m, last):
        rows = slice(0, last)
        acc = acc_v[m, rows, :]
        product = jnp.dot(
            (acc * u_v[m, rows, :].astype(f32)).astype(bf16), wout_v[...], preferred_element_type=f32
        )
        mean = jnp.mean(acc, axis=-1, keepdims=True)
        centred = acc - mean
        scale = lax.rsqrt(jnp.mean(centred * centred, axis=-1, keepdims=True) + mixed_eps)
        mixed = jnp.where(
            live_row[:last, :1] < val_ref[m, block], scale * (product - mean * gain_v[...]), 0.0
        )
        out_v[m, rows, :] = (x_v[m, rows, :].astype(f32) + mixed).astype(bf16)

    def finish(m, first, last):
        count = val_ref[m, block]
        for at in range(first, last, 128):
            rows = slice(at, at + 128)
            gated = normalise(acc_v[m, rows, :], mixed_eps) * u_v[m, rows, :].astype(f32)
            gated = jnp.where(live_row[:128] + at < count, gated, 0.0).astype(bf16)
            out_v[m, rows, :] = (
                x_v[m, rows, :].astype(f32)
                + jnp.dot(gated, wout_v[...], preferred_element_type=f32)
            ).astype(bf16)

    def settle():
        for m in range(micro):
            for p in range(len(parts(m))):
                if (m, p) != (final, len(parts(final)) - 1):
                    route(block < size - 1, m, p, lambda copy: copy.wait_send(), 0)
        for source, via, target, slot in detour_of:
            @pl.when(block == source)
            def _():
                leave(via, slot).wait_send()

            @pl.when(block == via)
            def _():
                forward(target, slot).wait_send()

    ready = []
    for m in range(micro):
        before = jnp.where(block > 0, val_ref[m, jnp.maximum(block - 1, 0)], 0)
        for p in range(len(parts(m))):
            first, last = parts(m)[p]
            rows = slice(first, last)

            if (m, first) == (final, 0):
                settle()
            route(block > 0, m, p, lambda copy: copy.wait_recv(), 1)

            if (m, first) == (final, 0):
                remote_part = raw_projection(xr_v[m, rows, :])
            else:
                norm_rows(xr_v, m, first, last)
                normed = norm_v[rows, :]

                def remote_part(c):
                    return jnp.dot(normed, win_v[c], preferred_element_type=f32)

            kp_v[rows, :] = silu(remote_part(3)).astype(bf16)
            value = silu(remote_part(1))
            vp_v[rows, :] = jnp.where(live_row[: last - first] + first < before, value, 0.0).astype(bf16)
            ahead = [(at, min(at + TILE, first), first, last) for at in range(0, first, TILE)]
            own = [(at, min(at + TILE, last), at, last) for at in range(first, last, TILE)]
            attend(m, True, own + ahead)
            for done in ready:
                finish(*done)
            ready = [(m, first, last)]
            if m == final and p == len(parts(m)) - 2:
                prepare(m, first)
    finish_last(final, tok // 4)
    route(block < size - 1, final, len(parts(final)) - 1, lambda copy: copy.wait_send(), 0)


def layer(x, w_in, w_out, lengths, valid):
    micro, tok, width = x.shape
    branch = w_out.shape[1]
    size = lax.axis_size("seq")
    assert tok == WINDOW
    planes = size // PLANE if lax.axis_size("pipe") == 1 else 0
    detours = max(planes - 1, 0)
    bf16 = jnp.bfloat16
    anywhere = pl.BlockSpec(memory_space=pl.ANY)
    return pl.pallas_call(
        functools.partial(layer_kernel, micro, size, detours),
        out_shape=pltpu.VMEM((micro, tok, width), bf16),
        in_specs=[anywhere] * 5,
        out_specs=pl.BlockSpec(memory_space=pltpu.VMEM),
        scratch_shapes=[
            pltpu.VMEM((micro, tok, width), bf16),
            pltpu.VMEM((micro, tok, width), bf16),
            pltpu.VMEM((4, width, branch), bf16),
            pltpu.VMEM((branch, width), bf16),
            pltpu.VMEM((tok, width), bf16),
            pltpu.VMEM((micro, tok, branch), bf16),
            pltpu.VMEM((tok, branch), bf16),
            pltpu.VMEM((micro, tok, branch), bf16),
            pltpu.VMEM((tok, branch), bf16),
            pltpu.VMEM((tok, branch), bf16),
            pltpu.VMEM((tok, branch), bf16),
            pltpu.VMEM((micro, tok, branch), jnp.float32),
            pltpu.VMEM((micro, tok, LANES), jnp.int32),
            pltpu.SMEM(lengths.shape, jnp.int32),
            pltpu.SMEM(valid.shape, jnp.int32),
            pltpu.VMEM((DETOUR * max(detours, 1), width), bf16),
            pltpu.VMEM((4, 8, branch), jnp.float32),
            pltpu.VMEM((tok // 4, width), jnp.float32),
            pltpu.SemaphoreType.DMA((micro,)),
            pltpu.SemaphoreType.DMA((5,)),
            pltpu.SemaphoreType.DMA((2,)),
            pltpu.SemaphoreType.DMA((micro, PARTS)),
            pltpu.SemaphoreType.DMA((micro, PARTS)),
            pltpu.SemaphoreType.DMA((2 + 2 * detours,)),
        ],
        compiler_params=pltpu.CompilerParams(
            collective_id=0, has_side_effects=True, vmem_limit_bytes=56 * 1024 * 1024
        ),
    )(x, w_in, w_out, lengths, valid)


def shards(inputs, w_in, w_out, lengths, valid):
    micro, tok, width = inputs.shape
    sections = lax.axis_size("pipe")
    if sections == 1:
        return layer(inputs, w_in, w_out, lengths, valid)[None]

    section = lax.axis_index("pipe")
    pairs = [(i, i + 1) for i in range(sections - 1)]

    def tick(step, carry):
        incoming, states = carry
        slot = step - section
        active = (slot >= 0) & (slot < micro)
        index = jnp.clip(slot, 0, micro - 1)
        fresh = lax.dynamic_index_in_dim(inputs, index, 0, keepdims=True)
        x_rows = jnp.where(section == 0, fresh, incoming)
        result = layer(
            x_rows,
            w_in,
            w_out,
            lax.dynamic_index_in_dim(lengths, index, 0, keepdims=True),
            lax.dynamic_index_in_dim(valid, index, 0, keepdims=True),
        )
        zero = jnp.zeros((), jnp.int32)
        updated = lax.dynamic_update_slice(states, result[None], (zero, index, zero, zero))
        states = jnp.where(active, updated, states)
        return (lax.ppermute(result, "pipe", pairs), states)

    start = (
        jnp.zeros((1, tok, width), jnp.bfloat16),
        jnp.zeros((1, micro, tok, width), jnp.bfloat16),
    )
    return lax.fori_loop(0, sections + micro - 1, tick, start)[1]


def solution(mesh):
    in_specs = (P(None, "seq", None), P("pipe", None, None), P("pipe", None, None), P(), P())
    out_specs = P("pipe", None, "seq", None)
    return jax.shard_map(shards, mesh=mesh, in_specs=in_specs, out_specs=out_specs, check_vma=False)
```

```python
import functools
import math

import jax
import jax.numpy as jnp
from jax import lax
from jax.experimental import pallas as pl
from jax.experimental.pallas import tpu as pltpu
from jax.sharding import PartitionSpec as P

HEAD_DIM = 128
WINDOW = 512
TILE = 256
LANES = 128
PARTS = 3
PLANE = 8
DETOUR = 80
VMEM_LIMIT = 40 * 1024 * 1024

norm_eps = 1e-05
out_eps = 0.001

score_scale = 1.0 / math.sqrt(HEAD_DIM)
fold = score_scale * 0.5
mixed_eps = out_eps * WINDOW


def normalise(values, epsilon):
    mean = jnp.mean(values, axis=-1, keepdims=True)
    centred = values - mean
    spread = jnp.mean(centred * centred, axis=-1, keepdims=True)
    return centred * lax.rsqrt(spread + epsilon)


def silu(v):
    half = v * 0.5
    return half + half * jnp.tanh(half)


def mask(low, previous, at, end, first, last, tok):
    shape = (end - at, last - first)
    low = jnp.concatenate([low] * (shape[1] // LANES), 1)
    place = lax.broadcasted_iota(jnp.int32, shape, 1) + (first - tok if previous else first)
    keep = place >= low
    line = lax.broadcasted_iota(jnp.int32, shape, 0) + at
    if previous:
        return keep & (place > line - tok) if first < end else keep
    return keep & (place <= line) if last > at else keep


def weigh(query, keys, keep):
    s = lax.dot_general(
        query, keys, (((1,), (1,)), ((), ())), preferred_element_type=jnp.float32
    )
    return jnp.where(keep, s + s * jnp.tanh(s), 0.0).astype(jnp.bfloat16)


def layer_kernel(
    micro, size, detours,
    x_hbm, win_hbm, wout_hbm, len_hbm, val_hbm,
    out_v, x_v, win_v, wout_v, u_v, q_v, acc_v, lo_v, sum_v, gain_v, last_v, live_v,
    xr_v, norm_v, v_v, k_v, kp_v, vp_v, len_ref, val_ref, detour_v,
    load_sem, weight_sem, scalar_sem, send_sem, recv_sem, detour_sem,
):
    block = lax.axis_index("seq")
    barrier = pltpu.get_barrier_semaphore()

    def greet(when, device):
        @pl.when(when)
        def _():
            pl.semaphore_signal(
                barrier, inc=1, device_id={"seq": device}, device_id_type=pl.DeviceIdType.MESH
            )

    greet(block > 0, block - 1)
    detour_of = [
        (z * PLANE + PLANE - 1, 0, z * PLANE + PLANE, z * DETOUR)
        for z in range(detours)
    ]
    for source, via, target, _ in detour_of:
        greet(block == target, via)
        greet(block == via, source)

    tok, width = x_v.shape[1], x_v.shape[2]
    branch = wout_v.shape[0]
    heads = branch // HEAD_DIM
    streams = len_ref.shape[1]
    f32 = jnp.float32
    bf16 = jnp.bfloat16

    loads = [
        pltpu.make_async_copy(x_hbm.at[m], x_v.at[m], load_sem.at[m]) for m in range(micro)
    ]
    weights = [
        pltpu.make_async_copy(
            win_hbm.at[0, :, pl.ds(c * branch, branch)], win_v.at[c], weight_sem.at[c]
        )
        for c in range(4)
    ]
    weights.append(pltpu.make_async_copy(wout_hbm.at[0], wout_v, weight_sem.at[4]))
    scalars = [
        pltpu.make_async_copy(len_hbm, len_ref, scalar_sem.at[0]),
        pltpu.make_async_copy(val_hbm, val_ref, scalar_sem.at[1]),
    ]
    for copy in loads + scalars + weights:
        copy.start()

    def parts(m):
        half, quarter = tok // 2, tok // 4
        if m < micro - 1:
            return [(half, tok), (0, half)]
        return [(half, tok), (quarter, half), (0, quarter)]

    def remote(src, dst, send, recv, device):
        return pltpu.make_async_remote_copy(
            src_ref=src,
            dst_ref=dst,
            send_sem=send,
            recv_sem=recv,
            device_id={"seq": device},
            device_id_type=pl.DeviceIdType.MESH,
        )

    def sends(m, p, cut=0):
        first, last = parts(m)[p]
        rows = pl.ds(first, last - cut - first)
        return remote(
            x_v.at[m, rows, :], xr_v.at[m, rows, :], send_sem.at[m, p], recv_sem.at[m, p], block + 1
        )

    final = micro - 1

    def leave(via, slot):
        rows = pl.ds(tok - DETOUR, DETOUR)
        return remote(
            x_v.at[final, rows, :], detour_v.at[pl.ds(slot, DETOUR), :],
            detour_sem.at[0], detour_sem.at[1 + slot // DETOUR], via,
        )

    def forward(target, slot):
        rows = pl.ds(tok - DETOUR, DETOUR)
        return remote(
            detour_v.at[pl.ds(slot, DETOUR), :], xr_v.at[final, rows, :],
            detour_sem.at[1 + detours + slot // DETOUR], detour_sem.at[1 + 2 * detours], target,
        )

    def route(when, m, p, act, end):
        plain = when
        if (m, p) == (final, 0):
            for source, via, target, slot in detour_of:
                here = block == (source if end == 0 else target)
                plain = plain & jnp.logical_not(here)

                @pl.when(here)
                def _():
                    act(sends(m, p, DETOUR))
                    if end:
                        act(forward(target, slot))

        @pl.when(plain)
        def _():
            act(sends(m, p))

    early = block < size - 1
    if detours:
        early = early & (block > 0)

    for m in range(micro):
        if m == 0:
            loads[0].wait()
            one = early
            for source, _, _, _ in detour_of:
                one = one & (block != source)

                @pl.when(block == source)
                def _():
                    pl.semaphore_wait(barrier, 2)

            @pl.when(one)
            def _():
                pl.semaphore_wait(barrier, 1)


        if m == final:
            pass
        if m > 0:
            loads[m].wait()
        if m == final:
            for source, via, _, slot in detour_of:
                @pl.when(block == source)
                def _():
                    leave(via, slot).start()

        for p in range(len(parts(m))):
            route(early, m, p, lambda copy: copy.start(), 0)

    @pl.when(block == 0)
    def _():
        xr_v[...] = jnp.zeros_like(xr_v)

    for copy in scalars + weights:
        copy.wait()
    row = lax.broadcasted_iota(jnp.int32, (tok, LANES), 0)
    for m in range(micro):
        place = row + block * tok
        start = jnp.zeros((tok, LANES), jnp.int32)
        bound = jnp.int32(0)
        for k in range(streams):
            bound = bound + len_ref[m, k]
            start = jnp.where(place >= bound, bound, start)
        lo_v[m] = start - block * tok

    def norm_rows(source, m, first=0, last=None):
        for at in range(first, tok if last is None else last, 128):
            rows = slice(at, at + 128)
            norm_v[rows, :] = normalise(source[m, rows, :].astype(f32), norm_eps).astype(bf16)

    live_row = lax.broadcasted_iota(jnp.int32, (tok, branch), 0)

    for c in (1, 3):
        ones = jnp.ones((8, width), bf16)
        sum_v[c] = jnp.dot(ones, win_v[c], preferred_element_type=f32)

    def project(c):
        return jnp.dot(norm_v[...], win_v[c], preferred_element_type=f32)

    def attend(m, previous, blocks):
        key_ref, value_ref = (kp_v, vp_v) if previous else (k_v, v_v)
        plans = []
        for h in range(heads):
            cols = slice(h * HEAD_DIM, (h + 1) * HEAD_DIM)
            for at, end, first, last in blocks:
                keep = mask(lo_v[m, at:end, :], previous, at, end, first, last, tok)
                plans.append((slice(at, end), cols, slice(first, last), keep))
        weights = [weigh(q_v[m, r, c], key_ref[k, c], keep) for r, c, k, keep in plans]
        for (r, c, k, _), a in zip(plans, weights):
            part = jnp.dot(a, value_ref[k, c], preferred_element_type=f32)
            acc_v[m, r, c] = acc_v[m, r, c] + part if previous else part

    for m in range(micro):
        norm_rows(x_v, m)
        count = val_ref[m, block]
        for c in (2, 3, 1, 0):
            part = silu(project(c))
            if c == 0:
                u_v[m] = part.astype(bf16)
            elif c == 1:
                v_v[...] = jnp.where(live_row < count, part, 0.0).astype(bf16)
            elif c == 2:
                q_v[m] = (part.astype(bf16).astype(f32) * fold).astype(bf16)
            else:
                k_v[...] = part.astype(bf16)
        attend(m, False, [(at, at + TILE, 0, at + TILE) for at in range(0, tok, TILE)])

    if detours:
        @pl.when(block == 0)
        def _():
            pl.semaphore_wait(barrier, 1 + detours)
            for m in range(micro):
                for p in range(len(parts(m))):
                    sends(m, p).start()
            for _, _, target, slot in detour_of:
                leave(0, slot).wait_recv()
                forward(target, slot).start()

    def prepare(m, last):
        rows = slice(0, last)
        acc = acc_v[m, rows, :]
        acc_v[m, rows, :] = acc - jnp.mean(acc, axis=-1, keepdims=True)
        gain_v[...] = jnp.dot(u_v[m, rows, :], wout_v[...], preferred_element_type=f32)

    def finish(m, first, last):
        count = val_ref[m, block]
        for at in range(first, last, 128):
            rows = slice(at, at + 128)
            gated = normalise(acc_v[m, rows, :], mixed_eps) * u_v[m, rows, :].astype(f32)
            gated = jnp.where(live_row[:128] + at < count, gated, 0.0).astype(bf16)
            out_v[m, rows, :] = (
                x_v[m, rows, :].astype(f32)
                + jnp.dot(gated, wout_v[...], preferred_element_type=f32)
            ).astype(bf16)

    def settle():
        for m in range(micro):
            for p in range(len(parts(m))):
                if (m, p) != (final, len(parts(final)) - 1):
                    route(block < size - 1, m, p, lambda copy: copy.wait_send(), 0)
        for source, via, target, slot in detour_of:
            @pl.when(block == source)
            def _():
                leave(via, slot).wait_send()

            @pl.when(block == via)
            def _():
                forward(target, slot).wait_send()

    ready = []
    for m in range(micro):
        before = jnp.where(block > 0, val_ref[m, jnp.maximum(block - 1, 0)], 0)
        for p in range(len(parts(m))):
            first, last = parts(m)[p]
            rows = slice(first, last)

            if (m, first) == (final, 0):
                settle()
                lane_row = lax.broadcasted_iota(jnp.int32, (last, LANES), 0)
                for slot, limit in enumerate((before, val_ref[m, block], val_ref[m, block] - last)):
                    live_v[slot] = (lane_row < limit).astype(jnp.int32)
            route(block > 0, m, p, lambda copy: copy.wait_recv(), 1)
            if (m, first) == (final, 0):
                last_v[...] = xr_v[m, rows, :]
                break

            norm_rows(xr_v, m, first, last)
            normed = norm_v[rows, :]
            kp_v[rows, :] = silu(
                jnp.dot(normed, win_v[3], preferred_element_type=f32)
            ).astype(bf16)
            value = silu(jnp.dot(normed, win_v[1], preferred_element_type=f32))
            vp_v[rows, :] = jnp.where(live_row[: last - first] + first < before, value, 0.0).astype(bf16)
            ahead = [(at, min(at + TILE, first), first, last) for at in range(0, first, TILE)]
            own = [(at, min(at + TILE, last), at, last) for at in range(first, last, TILE)]
            attend(m, True, own + ahead)
            for done in ready:
                finish(*done)
            ready = [(m, first, last)]
            if m == final and p == len(parts(m)) - 2:
                prepare(m, first)
    route(block < size - 1, final, len(parts(final)) - 1, lambda copy: copy.wait_send(), 0)


def tail_kernel(
    done_v, x_v, win_v, wout_v, u_v, q_v, acc_v, lo_v, sum_v, gain_v, last_v, live_v, out_hbm,
    tail_v, key_v, value_v, sem,
):
    micro, tok, width = x_v.shape
    m, last = micro - 1, last_v.shape[0]
    heads = wout_v.shape[0] // HEAD_DIM
    f32 = jnp.float32
    bf16 = jnp.bfloat16
    copies = [
        pltpu.make_async_copy(done_v.at[i], out_hbm.at[i], sem.at[i]) for i in range(m)
    ]
    rest = pl.ds(2 * last, tok - 2 * last)
    copies.append(pltpu.make_async_copy(done_v.at[m, rest, :], out_hbm.at[m, rest, :], sem.at[m]))
    for copy in copies:
        copy.start()

    def live(slot):
        return jnp.concatenate([live_v[slot]] * (width // LANES), 1) > 0

    raw = last_v[...].astype(f32)
    mean = jnp.mean(raw, axis=-1, keepdims=True)
    centred = raw - mean
    scale = lax.rsqrt(jnp.mean(centred * centred, axis=-1, keepdims=True) + norm_eps)

    def remote_part(c):
        product = jnp.dot(last_v[...], win_v[c], preferred_element_type=f32)
        return silu(scale * (product - mean * sum_v[c, 0:1, :]))

    key_v[...] = remote_part(3).astype(bf16)
    value_v[...] = jnp.where(live(0), remote_part(1), 0.0).astype(bf16)
    rows = slice(0, last)
    keep = mask(lo_v[m, rows, :], True, 0, last, 0, last, tok)
    columns = [slice(h * HEAD_DIM, (h + 1) * HEAD_DIM) for h in range(heads)]
    weights = [weigh(q_v[m, rows, c], key_v[:, c], keep) for c in columns]
    parts = [
        acc_v[m, rows, c] + jnp.dot(a, value_v[:, c], preferred_element_type=f32)
        for c, a in zip(columns, weights)
    ]

    after = slice(last, 2 * last)
    gated = normalise(acc_v[m, after, :], mixed_eps) * u_v[m, after, :].astype(f32)
    gated = jnp.where(live(2), gated, 0.0).astype(bf16)
    tail_v[after, :] = (
        x_v[m, after, :].astype(f32) + jnp.dot(gated, wout_v[...], preferred_element_type=f32)
    ).astype(bf16)

    acc = jnp.concatenate(parts, 1)
    product = jnp.dot(
        (acc * u_v[m, rows, :].astype(f32)).astype(bf16), wout_v[...], preferred_element_type=f32
    )
    middle = jnp.mean(acc, axis=-1, keepdims=True)
    centred = acc - middle
    spread = lax.rsqrt(jnp.mean(centred * centred, axis=-1, keepdims=True) + mixed_eps)
    mixed = jnp.where(live(1), spread * (product - middle * gain_v[...]), 0.0)
    tail_v[rows, :] = (x_v[m, rows, :].astype(f32) + mixed).astype(bf16)
    head = pl.ds(0, 2 * last)
    copies.append(pltpu.make_async_copy(tail_v, out_hbm.at[m, head, :], sem.at[micro]))
    copies[-1].start()
    for copy in copies:
        copy.wait()


def layer(x, w_in, w_out, lengths, valid):
    micro, tok, width = x.shape
    branch = w_out.shape[1]
    size = lax.axis_size("seq")
    assert tok == WINDOW
    planes = size // PLANE if lax.axis_size("pipe") == 1 else 0
    detours = max(planes - 1, 0)
    bf16 = jnp.bfloat16
    f32 = jnp.float32
    anywhere = pl.BlockSpec(memory_space=pl.ANY)
    local = pl.BlockSpec(memory_space=pltpu.VMEM)
    last = tok // 4
    kept = [
        pltpu.VMEM((micro, tok, width), bf16),
        pltpu.VMEM((micro, tok, width), bf16),
        pltpu.VMEM((4, width, branch), bf16),
        pltpu.VMEM((branch, width), bf16),
        pltpu.VMEM((micro, tok, branch), bf16),
        pltpu.VMEM((micro, tok, branch), bf16),
        pltpu.VMEM((micro, tok, branch), f32),
        pltpu.VMEM((micro, tok, LANES), jnp.int32),
        pltpu.VMEM((4, 8, branch), f32),
        pltpu.VMEM((last, width), f32),
        pltpu.VMEM((last, width), bf16),
        pltpu.VMEM((3, last, LANES), jnp.int32),
    ]
    state = pl.pallas_call(
        functools.partial(layer_kernel, micro, size, detours),
        out_shape=kept,
        in_specs=[anywhere] * 5,
        out_specs=[local] * len(kept),
        scratch_shapes=[
            pltpu.VMEM((micro, tok, width), bf16),
            pltpu.VMEM((tok, width), bf16),
            pltpu.VMEM((tok, branch), bf16),
            pltpu.VMEM((tok, branch), bf16),
            pltpu.VMEM((tok, branch), bf16),
            pltpu.VMEM((tok, branch), bf16),
            pltpu.SMEM(lengths.shape, jnp.int32),
            pltpu.SMEM(valid.shape, jnp.int32),
            pltpu.VMEM((DETOUR * max(detours, 1), width), bf16),
            pltpu.SemaphoreType.DMA((micro,)),
            pltpu.SemaphoreType.DMA((5,)),
            pltpu.SemaphoreType.DMA((2,)),
            pltpu.SemaphoreType.DMA((micro, PARTS)),
            pltpu.SemaphoreType.DMA((micro, PARTS)),
            pltpu.SemaphoreType.DMA((2 + 2 * detours,)),
        ],
        compiler_params=pltpu.CompilerParams(
            collective_id=0, has_side_effects=True, vmem_limit_bytes=VMEM_LIMIT
        ),
    )(*[
        pltpu.with_memory_space_constraint(array, pltpu.HBM)
        for array in (x, w_in, w_out, lengths, valid)
    ])
    return pl.pallas_call(
        tail_kernel,
        out_shape=jax.ShapeDtypeStruct((micro, tok, width), bf16),
        in_specs=[local] * len(kept),
        out_specs=anywhere,
        scratch_shapes=[
            pltpu.VMEM((2 * last, width), bf16),
            pltpu.VMEM((last, branch), bf16),
            pltpu.VMEM((last, branch), bf16),
            pltpu.SemaphoreType.DMA((micro + 1,)),
        ],
        compiler_params=pltpu.CompilerParams(vmem_limit_bytes=VMEM_LIMIT),
    )(*[pltpu.with_memory_space_constraint(array, pltpu.VMEM) for array in state])


def shards(inputs, w_in, w_out, lengths, valid):
    micro, tok, width = inputs.shape
    sections = lax.axis_size("pipe")
    if sections == 1:
        return layer(inputs, w_in, w_out, lengths, valid)[None]

    section = lax.axis_index("pipe")
    pairs = [(i, i + 1) for i in range(sections - 1)]

    def tick(step, carry):
        incoming, states = carry
        slot = step - section
        active = (slot >= 0) & (slot < micro)
        index = jnp.clip(slot, 0, micro - 1)
        fresh = lax.dynamic_index_in_dim(inputs, index, 0, keepdims=True)
        x_rows = jnp.where(section == 0, fresh, incoming)
        result = layer(
            x_rows,
            w_in,
            w_out,
            lax.dynamic_index_in_dim(lengths, index, 0, keepdims=True),
            lax.dynamic_index_in_dim(valid, index, 0, keepdims=True),
        )
        zero = jnp.zeros((), jnp.int32)
        updated = lax.dynamic_update_slice(states, result[None], (zero, index, zero, zero))
        states = jnp.where(active, updated, states)
        return (lax.ppermute(result, "pipe", pairs), states)

    start = (
        jnp.zeros((1, tok, width), jnp.bfloat16),
        jnp.zeros((1, micro, tok, width), jnp.bfloat16),
    )
    return lax.fori_loop(0, sections + micro - 1, tick, start)[1]


def solution(mesh):
    in_specs = (P(None, "seq", None), P("pipe", None, None), P("pipe", None, None), P(), P())
    out_specs = P("pipe", None, "seq", None)
    return jax.shard_map(shards, mesh=mesh, in_specs=in_specs, out_specs=out_specs, check_vma=False)
```

```python
import functools
import math

import jax
import jax.numpy as jnp
from jax import lax
from jax.experimental import pallas as pl
from jax.experimental.pallas import tpu as pltpu
from jax.sharding import PartitionSpec as P

HEAD_DIM = 128
WINDOW = 512
TILE = 256
LANES = 128
PARTS = 3
PLANE = 8
DETOUR = 80
VMEM_LIMIT = 40 * 1024 * 1024

norm_eps = 1e-05
out_eps = 0.001

score_scale = 1.0 / math.sqrt(HEAD_DIM)
fold = score_scale * 0.5
mixed_eps = out_eps * WINDOW


def normalise(values, epsilon):
    mean = jnp.mean(values, axis=-1, keepdims=True)
    centred = values - mean
    spread = jnp.mean(centred * centred, axis=-1, keepdims=True)
    return centred * lax.rsqrt(spread + epsilon)


def silu(v):
    half = v * 0.5
    return half + half * jnp.tanh(half)


def mask(low, previous, at, end, first, last, tok):
    shape = (end - at, last - first)
    low = jnp.concatenate([low] * (shape[1] // LANES), 1)
    place = lax.broadcasted_iota(jnp.int32, shape, 1) + (first - tok if previous else first)
    keep = place >= low
    line = lax.broadcasted_iota(jnp.int32, shape, 0) + at
    if previous:
        return keep & (place > line - tok) if first < end else keep
    return keep & (place <= line) if last > at else keep


def weigh(query, keys, keep):
    s = lax.dot_general(
        query, keys, (((1,), (1,)), ((), ())), preferred_element_type=jnp.float32
    )
    return jnp.where(keep, s + s * jnp.tanh(s), 0.0).astype(jnp.bfloat16)


def layer_kernel(
    micro, size, detours,
    x_hbm, win_hbm, wout_hbm, len_hbm, val_hbm,
    out_v, x_v, win_v, wout_v, u_v, q_v, acc_v, lo_v, sum_v, gain_v, last_v, live_v,
    xr_v, norm_v, v_v, k_v, kp_v, vp_v, len_ref, val_ref, detour_v,
    load_sem, weight_sem, scalar_sem, send_sem, recv_sem, detour_sem,
):
    block = lax.axis_index("seq")
    barrier = pltpu.get_barrier_semaphore()

    def greet(when, device):
        @pl.when(when)
        def _():
            pl.semaphore_signal(
                barrier, inc=1, device_id={"seq": device}, device_id_type=pl.DeviceIdType.MESH
            )

    greet(block > 0, block - 1)
    detour_of = [
        (z * PLANE + PLANE - 1, 0, z * PLANE + PLANE, z * DETOUR)
        for z in range(detours)
    ]
    for source, via, target, _ in detour_of:
        greet(block == target, via)
        greet(block == via, source)

    tok, width = x_v.shape[1], x_v.shape[2]
    branch = wout_v.shape[0]
    heads = branch // HEAD_DIM
    streams = len_ref.shape[1]
    f32 = jnp.float32
    bf16 = jnp.bfloat16

    loads = [
        pltpu.make_async_copy(x_hbm.at[m], x_v.at[m], load_sem.at[m]) for m in range(micro)
    ]
    weights = [
        pltpu.make_async_copy(
            win_hbm.at[0, :, pl.ds(c * branch, branch)], win_v.at[c], weight_sem.at[c]
        )
        for c in range(4)
    ]
    weights.append(pltpu.make_async_copy(wout_hbm.at[0], wout_v, weight_sem.at[4]))
    scalars = [
        pltpu.make_async_copy(len_hbm, len_ref, scalar_sem.at[0]),
        pltpu.make_async_copy(val_hbm, val_ref, scalar_sem.at[1]),
    ]
    for copy in loads + scalars + weights:
        copy.start()

    def parts(m):
        half, quarter = tok // 2, tok // 4
        if m < micro - 1:
            return [(half, tok), (0, half)]
        return [(half, tok), (quarter, half), (0, quarter)]

    def remote(src, dst, send, recv, device):
        return pltpu.make_async_remote_copy(
            src_ref=src,
            dst_ref=dst,
            send_sem=send,
            recv_sem=recv,
            device_id={"seq": device},
            device_id_type=pl.DeviceIdType.MESH,
        )

    def sends(m, p, cut=0):
        first, last = parts(m)[p]
        rows = pl.ds(first, last - cut - first)
        return remote(
            x_v.at[m, rows, :], xr_v.at[m, rows, :], send_sem.at[m, p], recv_sem.at[m, p], block + 1
        )

    final = micro - 1

    def leave(via, slot):
        rows = pl.ds(tok - DETOUR, DETOUR)
        return remote(
            x_v.at[final, rows, :], detour_v.at[pl.ds(slot, DETOUR), :],
            detour_sem.at[0], detour_sem.at[1 + slot // DETOUR], via,
        )

    def forward(target, slot):
        rows = pl.ds(tok - DETOUR, DETOUR)
        return remote(
            detour_v.at[pl.ds(slot, DETOUR), :], xr_v.at[final, rows, :],
            detour_sem.at[1 + detours + slot // DETOUR], detour_sem.at[1 + 2 * detours], target,
        )

    def route(when, m, p, act, end):
        plain = when
        if (m, p) == (final, 0):
            for source, via, target, slot in detour_of:
                here = block == (source if end == 0 else target)
                plain = plain & jnp.logical_not(here)

                @pl.when(here)
                def _():
                    act(sends(m, p, DETOUR))
                    if end:
                        act(forward(target, slot))

        @pl.when(plain)
        def _():
            act(sends(m, p))

    early = block < size - 1
    if detours:
        early = early & (block > 0)

    for m in range(micro):
        if m == 0:
            loads[0].wait()
            one = early
            for source, _, _, _ in detour_of:
                one = one & (block != source)

                @pl.when(block == source)
                def _():
                    pl.semaphore_wait(barrier, 2)

            @pl.when(one)
            def _():
                pl.semaphore_wait(barrier, 1)


        if m == final:
            pass
        if m > 0:
            loads[m].wait()
        if m == final:
            for source, via, _, slot in detour_of:
                @pl.when(block == source)
                def _():
                    leave(via, slot).start()

        for p in range(len(parts(m))):
            route(early, m, p, lambda copy: copy.start(), 0)

    @pl.when(block == 0)
    def _():
        xr_v[...] = jnp.zeros_like(xr_v)

    for copy in scalars + weights:
        copy.wait()
    row = lax.broadcasted_iota(jnp.int32, (tok, LANES), 0)
    for m in range(micro):
        place = row + block * tok
        start = jnp.zeros((tok, LANES), jnp.int32)
        bound = jnp.int32(0)
        for k in range(streams):
            bound = bound + len_ref[m, k]
            start = jnp.where(place >= bound, bound, start)
        lo_v[m] = start - block * tok

    def norm_rows(source, m, first=0, last=None):
        for at in range(first, tok if last is None else last, 128):
            rows = slice(at, at + 128)
            norm_v[rows, :] = normalise(source[m, rows, :].astype(f32), norm_eps).astype(bf16)

    live_row = lax.broadcasted_iota(jnp.int32, (tok, branch), 0)

    for c in (1, 3):
        ones = jnp.ones((8, width), bf16)
        sum_v[c] = jnp.dot(ones, win_v[c], preferred_element_type=f32)

    def project(c):
        return jnp.dot(norm_v[...], win_v[c], preferred_element_type=f32)

    def attend(m, previous, blocks):
        key_ref, value_ref = (kp_v, vp_v) if previous else (k_v, v_v)
        plans = []
        for h in range(heads):
            cols = slice(h * HEAD_DIM, (h + 1) * HEAD_DIM)
            for at, end, first, last in blocks:
                keep = mask(lo_v[m, at:end, :], previous, at, end, first, last, tok)
                plans.append((slice(at, end), cols, slice(first, last), keep))
        weights = [weigh(q_v[m, r, c], key_ref[k, c], keep) for r, c, k, keep in plans]
        for (r, c, k, _), a in zip(plans, weights):
            part = jnp.dot(a, value_ref[k, c], preferred_element_type=f32)
            acc_v[m, r, c] = acc_v[m, r, c] + part if previous else part

    for m in range(micro):
        norm_rows(x_v, m)
        count = val_ref[m, block]
        for c in (2, 3, 1, 0):
            part = silu(project(c))
            if c == 0:
                u_v[m] = part.astype(bf16)
            elif c == 1:
                v_v[...] = jnp.where(live_row < count, part, 0.0).astype(bf16)
            elif c == 2:
                q_v[m] = (part.astype(bf16).astype(f32) * fold).astype(bf16)
            else:
                k_v[...] = part.astype(bf16)
        attend(m, False, [(at, at + TILE, 0, at + TILE) for at in range(0, tok, TILE)])

    if detours:
        @pl.when(block == 0)
        def _():
            pl.semaphore_wait(barrier, 1 + detours)
            for m in range(micro):
                for p in range(len(parts(m))):
                    sends(m, p).start()
            for _, _, target, slot in detour_of:
                leave(0, slot).wait_recv()
                forward(target, slot).start()

    def prepare(m, last):
        rows = slice(0, last)
        acc = acc_v[m, rows, :]
        acc_v[m, rows, :] = acc - jnp.mean(acc, axis=-1, keepdims=True)
        gain_v[...] = jnp.dot(u_v[m, rows, :], wout_v[...], preferred_element_type=f32)

    def finish(m, first, last):
        count = val_ref[m, block]
        for at in range(first, last, 128):
            rows = slice(at, at + 128)
            gated = normalise(acc_v[m, rows, :], mixed_eps) * u_v[m, rows, :].astype(f32)
            gated = jnp.where(live_row[:128] + at < count, gated, 0.0).astype(bf16)
            out_v[m, rows, :] = (
                x_v[m, rows, :].astype(f32)
                + jnp.dot(gated, wout_v[...], preferred_element_type=f32)
            ).astype(bf16)

    def settle():
        for m in range(micro):
            for p in range(len(parts(m))):
                if (m, p) != (final, len(parts(final)) - 1):
                    route(block < size - 1, m, p, lambda copy: copy.wait_send(), 0)
        for source, via, target, slot in detour_of:
            @pl.when(block == source)
            def _():
                leave(via, slot).wait_send()

            @pl.when(block == via)
            def _():
                forward(target, slot).wait_send()

    ready = []
    for m in range(micro):
        before = jnp.where(block > 0, val_ref[m, jnp.maximum(block - 1, 0)], 0)
        for p in range(len(parts(m))):
            first, last = parts(m)[p]
            rows = slice(first, last)

            if (m, first) == (final, 0):
                settle()
                lane_row = lax.broadcasted_iota(jnp.int32, (last, LANES), 0)
                for slot, limit in enumerate((before, val_ref[m, block])):
                    live_v[slot] = (lane_row < limit).astype(jnp.int32)
            route(block > 0, m, p, lambda copy: copy.wait_recv(), 1)
            if (m, first) == (final, 0):
                last_v[...] = xr_v[m, rows, :]
                break

            norm_rows(xr_v, m, first, last)
            normed = norm_v[rows, :]
            kp_v[rows, :] = silu(
                jnp.dot(normed, win_v[3], preferred_element_type=f32)
            ).astype(bf16)
            value = silu(jnp.dot(normed, win_v[1], preferred_element_type=f32))
            vp_v[rows, :] = jnp.where(live_row[: last - first] + first < before, value, 0.0).astype(bf16)
            ahead = [(at, min(at + TILE, first), first, last) for at in range(0, first, TILE)]
            own = [(at, min(at + TILE, last), at, last) for at in range(first, last, TILE)]
            attend(m, True, own + ahead)
            for done in ready:
                finish(*done)
            ready = [(m, first, last)]
            if m == final and p == len(parts(m)) - 2:
                prepare(m, first)
                finish(*ready[0])
    route(block < size - 1, final, len(parts(final)) - 1, lambda copy: copy.wait_send(), 0)


def tail_kernel(
    done_v, x_v, win_v, wout_v, u_v, q_v, acc_v, lo_v, sum_v, gain_v, last_v, live_v, out_hbm,
    tail_v, key_v, value_v, sem,
):
    micro, tok, width = x_v.shape
    m, last = micro - 1, last_v.shape[0]
    heads = wout_v.shape[0] // HEAD_DIM
    f32 = jnp.float32
    bf16 = jnp.bfloat16
    copies = [
        pltpu.make_async_copy(done_v.at[i], out_hbm.at[i], sem.at[i]) for i in range(m)
    ]
    rest = pl.ds(last, tok - last)
    copies.append(pltpu.make_async_copy(done_v.at[m, rest, :], out_hbm.at[m, rest, :], sem.at[m]))
    for copy in copies:
        copy.start()

    def live(slot):
        return jnp.concatenate([live_v[slot]] * (width // LANES), 1) > 0

    raw = last_v[...].astype(f32)
    mean = jnp.mean(raw, axis=-1, keepdims=True)
    centred = raw - mean
    scale = lax.rsqrt(jnp.mean(centred * centred, axis=-1, keepdims=True) + norm_eps)

    def remote_part(c):
        product = jnp.dot(last_v[...], win_v[c], preferred_element_type=f32)
        return silu(scale * (product - mean * sum_v[c, 0:1, :]))

    key_v[...] = remote_part(3).astype(bf16)
    value_v[...] = jnp.where(live(0), remote_part(1), 0.0).astype(bf16)
    rows = slice(0, last)
    keep = mask(lo_v[m, rows, :], True, 0, last, 0, last, tok)
    columns = [slice(h * HEAD_DIM, (h + 1) * HEAD_DIM) for h in range(heads)]
    weights = [weigh(q_v[m, rows, c], key_v[:, c], keep) for c in columns]
    parts = [
        acc_v[m, rows, c] + jnp.dot(a, value_v[:, c], preferred_element_type=f32)
        for c, a in zip(columns, weights)
    ]

    acc = jnp.concatenate(parts, 1)
    product = jnp.dot(
        (acc * u_v[m, rows, :].astype(f32)).astype(bf16), wout_v[...], preferred_element_type=f32
    )
    middle = jnp.mean(acc, axis=-1, keepdims=True)
    centred = acc - middle
    spread = lax.rsqrt(jnp.mean(centred * centred, axis=-1, keepdims=True) + mixed_eps)
    mixed = jnp.where(live(1), spread * (product - middle * gain_v[...]), 0.0)
    tail_v[...] = (x_v[m, rows, :].astype(f32) + mixed).astype(bf16)
    head = pl.ds(0, last)
    copies.append(pltpu.make_async_copy(tail_v, out_hbm.at[m, head, :], sem.at[micro]))
    copies[-1].start()
    for copy in copies:
        copy.wait()


def layer(x, w_in, w_out, lengths, valid):
    micro, tok, width = x.shape
    branch = w_out.shape[1]
    size = lax.axis_size("seq")
    assert tok == WINDOW
    planes = size // PLANE if lax.axis_size("pipe") == 1 else 0
    detours = max(planes - 1, 0)
    bf16 = jnp.bfloat16
    f32 = jnp.float32
    anywhere = pl.BlockSpec(memory_space=pl.ANY)
    local = pl.BlockSpec(memory_space=pltpu.VMEM)
    last = tok // 4
    kept = [
        pltpu.VMEM((micro, tok, width), bf16),
        pltpu.VMEM((micro, tok, width), bf16),
        pltpu.VMEM((4, width, branch), bf16),
        pltpu.VMEM((branch, width), bf16),
        pltpu.VMEM((micro, tok, branch), bf16),
        pltpu.VMEM((micro, tok, branch), bf16),
        pltpu.VMEM((micro, tok, branch), f32),
        pltpu.VMEM((micro, tok, LANES), jnp.int32),
        pltpu.VMEM((4, 8, branch), f32),
        pltpu.VMEM((last, width), f32),
        pltpu.VMEM((last, width), bf16),
        pltpu.VMEM((2, last, LANES), jnp.int32),
    ]
    state = pl.pallas_call(
        functools.partial(layer_kernel, micro, size, detours),
        out_shape=kept,
        in_specs=[anywhere] * 5,
        out_specs=[local] * len(kept),
        scratch_shapes=[
            pltpu.VMEM((micro, tok, width), bf16),
            pltpu.VMEM((tok, width), bf16),
            pltpu.VMEM((tok, branch), bf16),
            pltpu.VMEM((tok, branch), bf16),
            pltpu.VMEM((tok, branch), bf16),
            pltpu.VMEM((tok, branch), bf16),
            pltpu.SMEM(lengths.shape, jnp.int32),
            pltpu.SMEM(valid.shape, jnp.int32),
            pltpu.VMEM((DETOUR * max(detours, 1), width), bf16),
            pltpu.SemaphoreType.DMA((micro,)),
            pltpu.SemaphoreType.DMA((5,)),
            pltpu.SemaphoreType.DMA((2,)),
            pltpu.SemaphoreType.DMA((micro, PARTS)),
            pltpu.SemaphoreType.DMA((micro, PARTS)),
            pltpu.SemaphoreType.DMA((2 + 2 * detours,)),
        ],
        compiler_params=pltpu.CompilerParams(
            collective_id=0, has_side_effects=True, vmem_limit_bytes=VMEM_LIMIT
        ),
    )(*[
        pltpu.with_memory_space_constraint(array, pltpu.HBM)
        for array in (x, w_in, w_out, lengths, valid)
    ])
    return pl.pallas_call(
        tail_kernel,
        out_shape=jax.ShapeDtypeStruct((micro, tok, width), bf16),
        in_specs=[local] * len(kept),
        out_specs=anywhere,
        scratch_shapes=[
            pltpu.VMEM((last, width), bf16),
            pltpu.VMEM((last, branch), bf16),
            pltpu.VMEM((last, branch), bf16),
            pltpu.SemaphoreType.DMA((micro + 1,)),
        ],
        compiler_params=pltpu.CompilerParams(vmem_limit_bytes=VMEM_LIMIT),
    )(*[pltpu.with_memory_space_constraint(array, pltpu.VMEM) for array in state])


def shards(inputs, w_in, w_out, lengths, valid):
    micro, tok, width = inputs.shape
    sections = lax.axis_size("pipe")
    if sections == 1:
        return layer(inputs, w_in, w_out, lengths, valid)[None]

    section = lax.axis_index("pipe")
    pairs = [(i, i + 1) for i in range(sections - 1)]

    def tick(step, carry):
        incoming, states = carry
        slot = step - section
        active = (slot >= 0) & (slot < micro)
        index = jnp.clip(slot, 0, micro - 1)
        fresh = lax.dynamic_index_in_dim(inputs, index, 0, keepdims=True)
        x_rows = jnp.where(section == 0, fresh, incoming)
        result = layer(
            x_rows,
            w_in,
            w_out,
            lax.dynamic_index_in_dim(lengths, index, 0, keepdims=True),
            lax.dynamic_index_in_dim(valid, index, 0, keepdims=True),
        )
        zero = jnp.zeros((), jnp.int32)
        updated = lax.dynamic_update_slice(states, result[None], (zero, index, zero, zero))
        states = jnp.where(active, updated, states)
        return (lax.ppermute(result, "pipe", pairs), states)

    start = (
        jnp.zeros((1, tok, width), jnp.bfloat16),
        jnp.zeros((1, micro, tok, width), jnp.bfloat16),
    )
    return lax.fori_loop(0, sections + micro - 1, tick, start)[1]


def solution(mesh):
    in_specs = (P(None, "seq", None), P("pipe", None, None), P("pipe", None, None), P(), P())
    out_specs = P("pipe", None, "seq", None)
    return jax.shard_map(shards, mesh=mesh, in_specs=in_specs, out_specs=out_specs, check_vma=False)
```

```python
import functools
import math

import jax
import jax.numpy as jnp
from jax import lax
from jax.experimental import pallas as pl
from jax.experimental.pallas import tpu as pltpu
from jax.sharding import PartitionSpec as P

HEAD_DIM = 128
WINDOW = 512
TILE = 256
LANES = 128
PARTS = 3
PLANE = 8
DETOUR = 96
VMEM_LIMIT = 40 * 1024 * 1024

norm_eps = 1e-05
out_eps = 0.001

score_scale = 1.0 / math.sqrt(HEAD_DIM)
fold = score_scale * 0.5
mixed_eps = out_eps * WINDOW


def normalise(values, epsilon):
    mean = jnp.mean(values, axis=-1, keepdims=True)
    centred = values - mean
    spread = jnp.mean(centred * centred, axis=-1, keepdims=True)
    return centred * lax.rsqrt(spread + epsilon)


def silu(v):
    half = v * 0.5
    return half + half * jnp.tanh(half)


def mask(low, previous, at, end, first, last, tok):
    shape = (end - at, last - first)
    low = jnp.concatenate([low] * (shape[1] // LANES), 1)
    place = lax.broadcasted_iota(jnp.int32, shape, 1) + (first - tok if previous else first)
    keep = place >= low
    line = lax.broadcasted_iota(jnp.int32, shape, 0) + at
    if previous:
        return keep & (place > line - tok) if first < end else keep
    return keep & (place <= line) if last > at else keep


def weigh(query, keys, keep):
    s = lax.dot_general(
        query, keys, (((1,), (1,)), ((), ())), preferred_element_type=jnp.float32
    )
    return jnp.where(keep, s + s * jnp.tanh(s), 0.0).astype(jnp.bfloat16)


def layer_kernel(
    micro, size, detours,
    x_hbm, win_hbm, wout_hbm, len_hbm, val_hbm,
    out_v, x_v, win_v, wout_v, u_v, q_v, acc_v, lo_v, sum_v, gain_v, last_v, live_v,
    xr_v, norm_v, v_v, k_v, kp_v, vp_v, len_ref, val_ref, detour_v,
    load_sem, weight_sem, scalar_sem, send_sem, recv_sem, detour_sem,
):
    block = lax.axis_index("seq")
    barrier = pltpu.get_barrier_semaphore()

    def greet(when, device):
        @pl.when(when)
        def _():
            pl.semaphore_signal(
                barrier, inc=1, device_id={"seq": device}, device_id_type=pl.DeviceIdType.MESH
            )

    greet(block > 0, block - 1)
    detour_of = [
        (z * PLANE + PLANE - 1, 0, z * PLANE + PLANE, z * DETOUR)
        for z in range(detours)
    ]
    for source, via, target, _ in detour_of:
        greet(block == target, via)
        greet(block == via, source)

    tok, width = x_v.shape[1], x_v.shape[2]
    branch = wout_v.shape[0]
    heads = branch // HEAD_DIM
    streams = len_ref.shape[1]
    f32 = jnp.float32
    bf16 = jnp.bfloat16

    loads = [
        pltpu.make_async_copy(x_hbm.at[m], x_v.at[m], load_sem.at[m]) for m in range(micro)
    ]
    weights = [
        pltpu.make_async_copy(
            win_hbm.at[0, :, pl.ds(c * branch, branch)], win_v.at[c], weight_sem.at[c]
        )
        for c in range(4)
    ]
    weights.append(pltpu.make_async_copy(wout_hbm.at[0], wout_v, weight_sem.at[4]))
    scalars = [
        pltpu.make_async_copy(len_hbm, len_ref, scalar_sem.at[0]),
        pltpu.make_async_copy(val_hbm, val_ref, scalar_sem.at[1]),
    ]
    for copy in loads + scalars + weights:
        copy.start()

    def parts(m):
        half, quarter = tok // 2, tok // 4
        if m < micro - 1:
            return [(half, tok), (0, half)]
        return [(half, tok), (quarter, half), (0, quarter)]

    def remote(src, dst, send, recv, device):
        return pltpu.make_async_remote_copy(
            src_ref=src,
            dst_ref=dst,
            send_sem=send,
            recv_sem=recv,
            device_id={"seq": device},
            device_id_type=pl.DeviceIdType.MESH,
        )

    def sends(m, p, cut=0):
        first, last = parts(m)[p]
        rows = pl.ds(first, last - cut - first)
        return remote(
            x_v.at[m, rows, :], xr_v.at[m, rows, :], send_sem.at[m, p], recv_sem.at[m, p], block + 1
        )

    final = micro - 1

    def leave(via, slot):
        rows = pl.ds(tok - DETOUR, DETOUR)
        return remote(
            x_v.at[final, rows, :], detour_v.at[pl.ds(slot, DETOUR), :],
            detour_sem.at[0], detour_sem.at[1 + slot // DETOUR], via,
        )

    def forward(target, slot):
        rows = pl.ds(tok - DETOUR, DETOUR)
        return remote(
            detour_v.at[pl.ds(slot, DETOUR), :], xr_v.at[final, rows, :],
            detour_sem.at[1 + detours + slot // DETOUR], detour_sem.at[1 + 2 * detours], target,
        )

    def route(when, m, p, act, end):
        plain = when
        if (m, p) == (final, 0):
            for source, via, target, slot in detour_of:
                here = block == (source if end == 0 else target)
                plain = plain & jnp.logical_not(here)

                @pl.when(here)
                def _():
                    act(sends(m, p, DETOUR))
                    if end:
                        act(forward(target, slot))

        @pl.when(plain)
        def _():
            act(sends(m, p))

    early = block < size - 1
    if detours:
        early = early & (block > 0)

    for m in range(micro):
        if m == 0:
            loads[0].wait()
            one = early
            for source, _, _, _ in detour_of:
                one = one & (block != source)

                @pl.when(block == source)
                def _():
                    pl.semaphore_wait(barrier, 2)

            @pl.when(one)
            def _():
                pl.semaphore_wait(barrier, 1)


        if m == final:
            pass
        if m > 0:
            loads[m].wait()
        if m == final:
            for source, via, _, slot in detour_of:
                @pl.when(block == source)
                def _():
                    leave(via, slot).start()

        for p in range(len(parts(m))):
            route(early, m, p, lambda copy: copy.start(), 0)

    @pl.when(block == 0)
    def _():
        xr_v[...] = jnp.zeros_like(xr_v)

    for copy in scalars + weights:
        copy.wait()
    row = lax.broadcasted_iota(jnp.int32, (tok, LANES), 0)
    for m in range(micro):
        place = row + block * tok
        start = jnp.zeros((tok, LANES), jnp.int32)
        bound = jnp.int32(0)
        for k in range(streams):
            bound = bound + len_ref[m, k]
            start = jnp.where(place >= bound, bound, start)
        lo_v[m] = start - block * tok

    def norm_rows(source, m, first=0, last=None):
        for at in range(first, tok if last is None else last, 128):
            rows = slice(at, at + 128)
            norm_v[rows, :] = normalise(source[m, rows, :].astype(f32), norm_eps).astype(bf16)

    live_row = lax.broadcasted_iota(jnp.int32, (tok, branch), 0)

    for c in (1, 3):
        ones = jnp.ones((8, width), bf16)
        sum_v[c] = jnp.dot(ones, win_v[c], preferred_element_type=f32)

    def project(c):
        return jnp.dot(norm_v[...], win_v[c], preferred_element_type=f32)

    def attend(m, previous, blocks):
        key_ref, value_ref = (kp_v, vp_v) if previous else (k_v, v_v)
        plans = []
        for h in range(heads):
            cols = slice(h * HEAD_DIM, (h + 1) * HEAD_DIM)
            for at, end, first, last in blocks:
                keep = mask(lo_v[m, at:end, :], previous, at, end, first, last, tok)
                plans.append((slice(at, end), cols, slice(first, last), keep))
        weights = [weigh(q_v[m, r, c], key_ref[k, c], keep) for r, c, k, keep in plans]
        for (r, c, k, _), a in zip(plans, weights):
            part = jnp.dot(a, value_ref[k, c], preferred_element_type=f32)
            acc_v[m, r, c] = acc_v[m, r, c] + part if previous else part

    for m in range(micro):
        norm_rows(x_v, m)
        count = val_ref[m, block]
        for c in (2, 3, 1, 0):
            part = silu(project(c))
            if c == 0:
                u_v[m] = part.astype(bf16)
            elif c == 1:
                v_v[...] = jnp.where(live_row < count, part, 0.0).astype(bf16)
            elif c == 2:
                q_v[m] = (part.astype(bf16).astype(f32) * fold).astype(bf16)
            else:
                k_v[...] = part.astype(bf16)
        attend(m, False, [(at, at + TILE, 0, at + TILE) for at in range(0, tok, TILE)])

    if detours:
        @pl.when(block == 0)
        def _():
            pl.semaphore_wait(barrier, 1 + detours)
            for m in range(micro):
                for p in range(len(parts(m))):
                    sends(m, p).start()
            for _, _, target, slot in detour_of:
                leave(0, slot).wait_recv()
                forward(target, slot).start()

    def prepare(m, last):
        rows = slice(0, last)
        acc = acc_v[m, rows, :]
        acc_v[m, rows, :] = acc - jnp.mean(acc, axis=-1, keepdims=True)
        gain_v[...] = jnp.dot(u_v[m, rows, :], wout_v[...], preferred_element_type=f32)

    def finish(m, first, last):
        count = val_ref[m, block]
        for at in range(first, last, 128):
            rows = slice(at, at + 128)
            gated = normalise(acc_v[m, rows, :], mixed_eps) * u_v[m, rows, :].astype(f32)
            gated = jnp.where(live_row[:128] + at < count, gated, 0.0).astype(bf16)
            out_v[m, rows, :] = (
                x_v[m, rows, :].astype(f32)
                + jnp.dot(gated, wout_v[...], preferred_element_type=f32)
            ).astype(bf16)

    def settle():
        for m in range(micro):
            for p in range(len(parts(m))):
                if (m, p) != (final, len(parts(final)) - 1):
                    route(block < size - 1, m, p, lambda copy: copy.wait_send(), 0)
        for source, via, target, slot in detour_of:
            @pl.when(block == source)
            def _():
                leave(via, slot).wait_send()

            @pl.when(block == via)
            def _():
                forward(target, slot).wait_send()

    ready = []
    for m in range(micro):
        before = jnp.where(block > 0, val_ref[m, jnp.maximum(block - 1, 0)], 0)
        for p in range(len(parts(m))):
            first, last = parts(m)[p]
            rows = slice(first, last)

            if (m, first) == (final, 0):
                settle()
                lane_row = lax.broadcasted_iota(jnp.int32, (last, LANES), 0)
                for slot, limit in enumerate((before, val_ref[m, block])):
                    live_v[slot] = (lane_row < limit).astype(jnp.int32)
            route(block > 0, m, p, lambda copy: copy.wait_recv(), 1)
            if (m, first) == (final, 0):
                last_v[...] = xr_v[m, rows, :]
                break

            norm_rows(xr_v, m, first, last)
            normed = norm_v[rows, :]
            kp_v[rows, :] = silu(
                jnp.dot(normed, win_v[3], preferred_element_type=f32)
            ).astype(bf16)
            value = silu(jnp.dot(normed, win_v[1], preferred_element_type=f32))
            vp_v[rows, :] = jnp.where(live_row[: last - first] + first < before, value, 0.0).astype(bf16)
            ahead = [(at, min(at + TILE, first), first, last) for at in range(0, first, TILE)]
            own = [(at, min(at + TILE, last), at, last) for at in range(first, last, TILE)]
            attend(m, True, own + ahead)
            for done in ready:
                finish(*done)
            ready = [(m, first, last)]
            if m == final and p == len(parts(m)) - 2:
                prepare(m, first)
                finish(*ready[0])
    route(block < size - 1, final, len(parts(final)) - 1, lambda copy: copy.wait_send(), 0)


def tail_kernel(
    done_v, x_v, win_v, wout_v, u_v, q_v, acc_v, lo_v, sum_v, gain_v, last_v, live_v, out_hbm,
    tail_v, key_v, value_v, sem,
):
    micro, tok, width = x_v.shape
    m, last = micro - 1, last_v.shape[0]
    heads = wout_v.shape[0] // HEAD_DIM
    f32 = jnp.float32
    bf16 = jnp.bfloat16
    copies = [
        pltpu.make_async_copy(done_v.at[i], out_hbm.at[i], sem.at[i]) for i in range(m)
    ]
    rest = pl.ds(last, tok - last)
    copies.append(pltpu.make_async_copy(done_v.at[m, rest, :], out_hbm.at[m, rest, :], sem.at[m]))
    for copy in copies:
        copy.start()

    def live(slot):
        return jnp.concatenate([live_v[slot]] * (width // LANES), 1) > 0

    raw = last_v[...].astype(f32)
    mean = jnp.mean(raw, axis=-1, keepdims=True)
    centred = raw - mean
    scale = lax.rsqrt(jnp.mean(centred * centred, axis=-1, keepdims=True) + norm_eps)

    def remote_part(c):
        product = jnp.dot(last_v[...], win_v[c], preferred_element_type=f32)
        return silu(scale * (product - mean * sum_v[c, 0:1, :]))

    key_v[...] = remote_part(3).astype(bf16)
    value_v[...] = jnp.where(live(0), remote_part(1), 0.0).astype(bf16)
    rows = slice(0, last)
    keep = mask(lo_v[m, rows, :], True, 0, last, 0, last, tok)
    columns = [slice(h * HEAD_DIM, (h + 1) * HEAD_DIM) for h in range(heads)]
    weights = [weigh(q_v[m, rows, c], key_v[:, c], keep) for c in columns]
    parts = [
        acc_v[m, rows, c] + jnp.dot(a, value_v[:, c], preferred_element_type=f32)
        for c, a in zip(columns, weights)
    ]

    acc = jnp.concatenate(parts, 1)
    product = jnp.dot(
        (acc * u_v[m, rows, :].astype(f32)).astype(bf16), wout_v[...], preferred_element_type=f32
    )
    middle = jnp.mean(acc, axis=-1, keepdims=True)
    square = jnp.mean(acc * acc, axis=-1, keepdims=True) - middle * middle
    spread = lax.rsqrt(jnp.maximum(square, 0.0) + mixed_eps)
    mixed = jnp.where(live(1), spread * (product - middle * gain_v[...]), 0.0)
    tail_v[...] = (x_v[m, rows, :].astype(f32) + mixed).astype(bf16)
    head = pl.ds(0, last)
    copies.append(pltpu.make_async_copy(tail_v, out_hbm.at[m, head, :], sem.at[micro]))
    copies[-1].start()
    for copy in copies:
        copy.wait()


def layer(x, w_in, w_out, lengths, valid):
    micro, tok, width = x.shape
    branch = w_out.shape[1]
    size = lax.axis_size("seq")
    assert tok == WINDOW
    planes = size // PLANE if lax.axis_size("pipe") == 1 else 0
    detours = max(planes - 1, 0)
    bf16 = jnp.bfloat16
    f32 = jnp.float32
    anywhere = pl.BlockSpec(memory_space=pl.ANY)
    local = pl.BlockSpec(memory_space=pltpu.VMEM)
    last = tok // 4
    kept = [
        pltpu.VMEM((micro, tok, width), bf16),
        pltpu.VMEM((micro, tok, width), bf16),
        pltpu.VMEM((4, width, branch), bf16),
        pltpu.VMEM((branch, width), bf16),
        pltpu.VMEM((micro, tok, branch), bf16),
        pltpu.VMEM((micro, tok, branch), bf16),
        pltpu.VMEM((micro, tok, branch), f32),
        pltpu.VMEM((micro, tok, LANES), jnp.int32),
        pltpu.VMEM((4, 8, branch), f32),
        pltpu.VMEM((last, width), f32),
        pltpu.VMEM((last, width), bf16),
        pltpu.VMEM((2, last, LANES), jnp.int32),
    ]
    state = pl.pallas_call(
        functools.partial(layer_kernel, micro, size, detours),
        out_shape=kept,
        in_specs=[anywhere] * 5,
        out_specs=[local] * len(kept),
        scratch_shapes=[
            pltpu.VMEM((micro, tok, width), bf16),
            pltpu.VMEM((tok, width), bf16),
            pltpu.VMEM((tok, branch), bf16),
            pltpu.VMEM((tok, branch), bf16),
            pltpu.VMEM((tok, branch), bf16),
            pltpu.VMEM((tok, branch), bf16),
            pltpu.SMEM(lengths.shape, jnp.int32),
            pltpu.SMEM(valid.shape, jnp.int32),
            pltpu.VMEM((DETOUR * max(detours, 1), width), bf16),
            pltpu.SemaphoreType.DMA((micro,)),
            pltpu.SemaphoreType.DMA((5,)),
            pltpu.SemaphoreType.DMA((2,)),
            pltpu.SemaphoreType.DMA((micro, PARTS)),
            pltpu.SemaphoreType.DMA((micro, PARTS)),
            pltpu.SemaphoreType.DMA((2 + 2 * detours,)),
        ],
        compiler_params=pltpu.CompilerParams(
            collective_id=0, has_side_effects=True, vmem_limit_bytes=VMEM_LIMIT
        ),
    )(*[
        pltpu.with_memory_space_constraint(array, pltpu.HBM)
        for array in (x, w_in, w_out, lengths, valid)
    ])
    return pl.pallas_call(
        tail_kernel,
        out_shape=jax.ShapeDtypeStruct((micro, tok, width), bf16),
        in_specs=[local] * len(kept),
        out_specs=anywhere,
        scratch_shapes=[
            pltpu.VMEM((last, width), bf16),
            pltpu.VMEM((last, branch), bf16),
            pltpu.VMEM((last, branch), bf16),
            pltpu.SemaphoreType.DMA((micro + 1,)),
        ],
        compiler_params=pltpu.CompilerParams(vmem_limit_bytes=VMEM_LIMIT),
    )(*[pltpu.with_memory_space_constraint(array, pltpu.VMEM) for array in state])


def shards(inputs, w_in, w_out, lengths, valid):
    micro, tok, width = inputs.shape
    sections = lax.axis_size("pipe")
    if sections == 1:
        return layer(inputs, w_in, w_out, lengths, valid)[None]

    section = lax.axis_index("pipe")
    pairs = [(i, i + 1) for i in range(sections - 1)]

    def tick(step, carry):
        incoming, states = carry
        slot = step - section
        active = (slot >= 0) & (slot < micro)
        index = jnp.clip(slot, 0, micro - 1)
        fresh = lax.dynamic_index_in_dim(inputs, index, 0, keepdims=True)
        x_rows = jnp.where(section == 0, fresh, incoming)
        result = layer(
            x_rows,
            w_in,
            w_out,
            lax.dynamic_index_in_dim(lengths, index, 0, keepdims=True),
            lax.dynamic_index_in_dim(valid, index, 0, keepdims=True),
        )
        zero = jnp.zeros((), jnp.int32)
        updated = lax.dynamic_update_slice(states, result[None], (zero, index, zero, zero))
        states = jnp.where(active, updated, states)
        return (lax.ppermute(result, "pipe", pairs), states)

    start = (
        jnp.zeros((1, tok, width), jnp.bfloat16),
        jnp.zeros((1, micro, tok, width), jnp.bfloat16),
    )
    return lax.fori_loop(0, sections + micro - 1, tick, start)[1]


def solution(mesh):
    in_specs = (P(None, "seq", None), P("pipe", None, None), P("pipe", None, None), P(), P())
    out_specs = P("pipe", None, "seq", None)
    return jax.shard_map(shards, mesh=mesh, in_specs=in_specs, out_specs=out_specs, check_vma=False)
```
